512 devices in a mesh: fsdp: 16 (over x, z_hi), tensor: 8 (over z_lo, core), pool: 4 (over y).
Axes of the slice: x: 4, y: 4, z: 16 (z_hi: 4, z_lo: 4; z = z_hi * 4 + z_lo), core: 2. Of those that a mesh axis runs over, the one named last changes fastest.
Arguments:
- hidden: bfloat16 [32768, 5120], P(('fsdp', 'pool'), 'tensor'), may hold values from -6 to 6
- queries: bfloat16 [32768, 5120], P(('fsdp', 'pool'), 'tensor'), may hold values from -200 to 200
- cotangent: bfloat16 [32768, 5120], P(('fsdp', 'pool'), 'tensor'), may hold values from -6 to 6
- segment: int32 [64, 512], P(('fsdp', 'pool')), may hold values from 0 to 15, never falling along the last dimension, each value on 1 to 384 neighbouring positions
- clip_mask: int32 [32768], P(('fsdp', 'pool')), may hold values 0 or 1
- rewards: float32 [1024], P(('fsdp', 'pool')), may hold values from 0 to 1
- seq_order: int32 [1024], P(('fsdp', 'pool')), may hold values from 0 to 1023, each once
- kv_weight: float32 [5120, 2, 1024], P('fsdp', None, 'tensor'), may hold values from -0.078125 to 0.078125
- moment_one: float32 [5120, 2, 1024], P('fsdp', None, 'tensor'), may hold values from -60 to 60
- moment_two: float32 [5120, 2, 1024], P('fsdp', None, 'tensor'), may hold values from 1 to 10000
- dec_hidden: bfloat16 [512, 4, 5120], P(('fsdp', 'pool')), may hold values from -6 to 6
- dec_queries: bfloat16 [512, 4, 5120], P(('fsdp', 'pool'), None, 'tensor'), may hold values from -200 to 200
- kv_cache: bfloat16 [512, 256, 2, 1024], P(('fsdp', 'pool'), None, None, 'tensor'), may hold values from -6 to 6
- cache_len: int32 [512], P(('fsdp', 'pool')), may hold values from 1 to 256
Outputs:
- new_weight: float32 [5120, 2, 1024], P('fsdp', None, 'tensor')
- new_moment_one: float32 [5120, 2, 1024], P('fsdp', None, 'tensor')
- new_moment_two: float32 [5120, 2, 1024], P('fsdp', None, 'tensor')
- dec_out: bfloat16 [512, 4, 5120], P(('fsdp', 'pool'), None, 'tensor')
The draws below stay inside these ranges and needn't reach their ends.
Inputs may be any that keep to these rules, and one draw needn't show every extreme that they name: `segment`: each row never falls; every sequence number of a row has 1 to 384 tokens. `seq_order`: each place once.
All inputs are finite; a program needn't handle non-finite values. No bound on the sum of `clip_mask` on one device may be relied on, other than what follows from the above.
Results may differ from the reference program's by a relative error of at most 0.014.
The reference program's roundings to bfloat16 on the way count: a program that leaves them out, or rounds other values in their place, can miss the bound.
Values may be sent and summed in bfloat16 or wider, within the bound.
A program may use at most 64 MiB of HBM per device.

```python
import math
import jax
import jax.numpy as jnp
import numpy as np
from jax import lax

D = 5120
QH = 40
KVH = 8
HD = 128
TOK_DEV = 512
GROUP = 16
CACHE = 256
STEPS = 4
SEQ_DEV = 16
SHARDS = 64
TOKENS = 32768
SEQS = 1024
REQ = 512


def query_law(key, rows, columns):
    base = jax.random.normal(key, (rows, columns), jnp.float32)
    return jnp.clip(base, -200.0, 200.0)


def draw_queries(key, part):
    return query_law(jax.random.fold_in(key, 11), TOKENS, QH * HD).astype(jnp.bfloat16)


def draw_dec_queries(key, part):
    table = query_law(jax.random.fold_in(key, 13), REQ * STEPS, QH * HD)
    return table.reshape(REQ, STEPS, QH * HD).astype(jnp.bfloat16)


def with_ends(result, stream_key, low, high):
    place = [jax.random.randint(jax.random.fold_in(stream_key, axis), (), 0, length) for axis, length in enumerate(result.shape)]
    widest = result.shape.index(max(result.shape))
    next_to = place[:widest] + [(place[widest] + 1) % result.shape[widest]] + place[widest + 1:]
    return result.at[tuple(place)].set(low).at[tuple(next_to)].set(high)


def level_of(key, dims, cuts, least, top_value):
    gain = 1.0
    for dim, blocks in cuts:
        draws = jax.random.uniform(jax.random.fold_in(jax.random.fold_in(key, 6), dim), (blocks,), jnp.float32, least / len(cuts), top_value / len(cuts))
        gain = gain * jnp.repeat(jnp.exp(draws), dims[dim] // blocks).reshape((-1,) + (1,) * (len(dims) - 1 - dim))
    return gain


def profile(number_of, total, most, skew):
    portions = [(1 << 20) // math.isqrt(rank ** skew) + 1 for rank in range(2, number_of + 1)]
    spare, holding = total - most - (number_of - 1), [1] * (number_of - 1)
    while spare > 0:
        free = [i for i in range(number_of - 1) if holding[i] < most]
        pool, left = sum([portions[i] for i in free]), spare
        for i in free:
            extra = min(most - holding[i], max(1, left * portions[i] // pool), spare)
            holding[i] = holding[i] + extra
            spare = spare - extra
    return np.array([most] + holding)


def ragged(rng, count, total, most, lean):
    if count == 2:
        one = jax.random.randint(rng, (), max(1, total - most), min(most, total - 1) + 1)
        return jnp.stack([one, total - one])
    sizes = jnp.asarray(profile(count, total, most, lean), jnp.int32)
    twos = (count - 1) // 2
    giver, taker = sizes[1:1 + 2 * twos:2], sizes[2:2 + 2 * twos:2]
    room = jnp.minimum(giver - 1, most - taker)
    moved = jax.random.randint(jax.random.fold_in(rng, 1), (twos,), 0, 1 << 20) % (room + 1)
    sizes = sizes.at[1:1 + 2 * twos:2].set(giver - moved).at[2:2 + 2 * twos:2].set(taker + moved)
    return sizes[jax.random.permutation(jax.random.fold_in(rng, 2), count)]


def noise(own_key, extent, width, limit, cuts=(), kind=jnp.bfloat16):
    drawn = jax.random.normal(own_key, extent, jnp.float32) * width
    if len(cuts) > 0:
        drawn = level_of(own_key, extent, cuts, -0.22, 0.18) * drawn
    return jnp.clip(drawn, min=-limit, max=limit).astype(kind)


def setup_inputs(seed: int = 0) -> dict:
    splits = jax.random.split(jax.random.key(seed), 15)
    hidden = noise(splits[0], (TOKENS, D), 1.0, 6.0, ((0, 64), (1, 8)))
    queries = draw_queries(jax.random.fold_in(splits[14], 71), 0)
    cotangent = noise(splits[2], (TOKENS, QH * HD), 1.0, 6.0, ((0, 64), (1, 8)))
    segment = jax.vmap(lambda own: jnp.searchsorted(jnp.cumsum(ragged(own, SEQ_DEV, TOK_DEV, 3 * TOK_DEV // 4, 0)), jnp.arange(TOK_DEV), side="right"))(jax.random.split(splits[3], SHARDS)).reshape((SHARDS, TOK_DEV)).astype(jnp.int32)
    clip_mask = with_ends((jax.random.randint(splits[4], (TOKENS,), 0, 4) < 3).astype(jnp.int32), jax.random.fold_in(splits[4], 1), 0, 1)
    rewards = jnp.clip(1.0 * jax.random.uniform(splits[5], (SEQS,), jnp.float32) ** level_of(splits[5], (SEQS,), ((0, 64),), -0.2, 0.2), 0.0, 1.0)
    seq_order = jax.random.permutation(splits[6], SEQS).astype(jnp.int32)
    kv_weight = noise(splits[7], (D, 2, KVH * HD), D ** -0.5, 0.078125, ((0, 16), (2, 8)), jnp.float32)
    moment_one = noise(splits[8], (D, 2, KVH * HD), 10.0, 60.0, ((0, 16), (2, 8)), jnp.float32)
    moment_two = jnp.clip(jnp.exp(math.log(10000.0) - 9.2103404 * jax.random.uniform(splits[9], (D, 2, KVH * HD), jnp.float32) ** level_of(splits[9], (D, 2, KVH * HD), ((0, 16), (2, 8)), -0.2, 0.2)), 1.0, 10000.0)
    dec_hidden = noise(splits[10], (REQ, STEPS, D), 1.0, 6.0, ((0, 64),))
    dec_queries = draw_dec_queries(jax.random.fold_in(splits[14], 71), 0)
    kv_cache = noise(splits[12], (REQ, CACHE, 2, KVH * HD), 1.0, 6.0, ((0, 64), (3, 8)))
    cache_len = with_ends(jax.random.randint(splits[13], (REQ,), 1, CACHE + 1), jax.random.fold_in(splits[13], 1), 1, CACHE).astype(jnp.int32)
    return dict(hidden=hidden, queries=queries, cotangent=cotangent, segment=segment, clip_mask=clip_mask, rewards=rewards, seq_order=seq_order, kv_weight=kv_weight, moment_one=moment_one, moment_two=moment_two, dec_hidden=dec_hidden, dec_queries=dec_queries, kv_cache=kv_cache, cache_len=cache_len)


beta_one = 0.9
beta_two = 0.999
learn_rate = 0.001
weight_decay = 0.1
adam_epsilon = 1e-08
adam_step = 10.0
variance_floor = 0.04
masked_score = -1e+30

def rounded(value):
    return lax.optimization_barrier(value.astype(jnp.bfloat16)).astype(jnp.float32)

def learner_grads(keys_values, queries, cotangent, segment, coefficient):
    block_rows = queries.shape[0]
    head_size = queries.shape[3]
    score_scale = 1.0 / math.sqrt(head_size)
    key_rows = keys_values[:, 0].astype(jnp.float32)
    value_rows = keys_values[:, 1].astype(jnp.float32)
    query_full = queries.astype(jnp.float32)
    scores = jnp.einsum('thrd,uhd->hrtu', query_full, key_rows) * score_scale
    places = jnp.arange(block_rows)
    allowed = (segment[:, None] == segment[None, :]) & (places[None, :] <= places[:, None])
    scores = jnp.where(allowed, scores, masked_score)
    row_max = lax.optimization_barrier(jnp.max(scores, axis=-1, keepdims=True))
    weights = jnp.exp(scores - row_max)
    attention = weights / lax.optimization_barrier(jnp.sum(weights, axis=-1, keepdims=True))
    attention_low = rounded(attention)
    upstream = rounded(coefficient[:, None, None, None] * cotangent.astype(jnp.float32))
    grad_prob = jnp.einsum('thrd,uhd->hrtu', upstream, value_rows)
    row_inner = lax.optimization_barrier(jnp.sum(attention * grad_prob, axis=-1, keepdims=True))
    grad_score = rounded(attention * (grad_prob - row_inner) * score_scale)
    grad_values = jnp.einsum('hrtu,thrd->uhd', attention_low, upstream)
    grad_keys = jnp.einsum('hrtu,thrd->uhd', grad_score, query_full)
    return jnp.stack([grad_keys, grad_values], axis=1).astype(jnp.bfloat16)

def decode_attend(queries, cache, fresh, lengths):
    head_size = queries.shape[4]
    steps_here = queries.shape[1]
    capacity = cache.shape[1]
    score_scale = 1.0 / math.sqrt(head_size)
    query_full = queries.astype(jnp.float32)
    cached = jnp.einsum('bshqd,blhd->bshql', query_full, cache[:, :, 0].astype(jnp.float32)) * score_scale
    recent = jnp.einsum('bshqd,bjhd->bshqj', query_full, fresh[:, :, 0].astype(jnp.float32)) * score_scale
    live = jnp.arange(capacity)[None, :] < lengths[:, None]
    cached = jnp.where(live[:, None, None, None, :], cached, masked_score)
    before = jnp.arange(steps_here)[None, :] <= jnp.arange(steps_here)[:, None]
    recent = jnp.where(before[None, :, None, None, :], recent, masked_score)
    row_max = jnp.maximum(lax.optimization_barrier(jnp.max(cached, axis=-1, keepdims=True)), lax.optimization_barrier(jnp.max(recent, axis=-1, keepdims=True)))
    cached_exp = jnp.exp(cached - row_max)
    recent_exp = jnp.exp(recent - row_max)
    total = lax.optimization_barrier(jnp.sum(cached_exp, axis=-1, keepdims=True)) + lax.optimization_barrier(jnp.sum(recent_exp, axis=-1, keepdims=True))
    cached_low = rounded(cached_exp / total)
    recent_low = rounded(recent_exp / total)
    output = jnp.einsum('bshql,blhd->bshqd', cached_low, cache[:, :, 1].astype(jnp.float32))
    output = output + jnp.einsum('bshqj,bjhd->bshqd', recent_low, fresh[:, :, 1].astype(jnp.float32))
    return output.astype(jnp.bfloat16).reshape(queries.shape[0], steps_here, -1)

def reference(hidden, queries, cotangent, segment, clip_mask, rewards, seq_order, kv_weight, moment_one, moment_two, dec_hidden, dec_queries, kv_cache, cache_len):
    blocks = segment.shape[0]
    tok_rows = segment.shape[1]
    seq_rows = rewards.shape[0] // blocks
    groups_total = rewards.shape[0] // GROUP
    kv_width = kv_weight.shape[2]
    heads_kv = kv_width // HD
    head_ratio = QH // KVH
    group_of = seq_order // GROUP
    onehot = (group_of[:, None] == jnp.arange(groups_total, dtype=jnp.int32)[None, :]).astype(jnp.float32)
    stats = jnp.stack([rewards, rewards * rewards], axis=1)
    sums = lax.optimization_barrier(jnp.sum(onehot[:, :, None] * stats[:, None, :], axis=0))
    mean = sums[:, 0] / GROUP
    spread = sums[:, 1] / GROUP - mean * mean
    denom = jnp.sqrt(jnp.maximum(spread, variance_floor))
    advantage = (rewards - lax.optimization_barrier(jnp.sum(onehot * mean[None, :], axis=1))) / lax.optimization_barrier(jnp.sum(onehot * denom[None, :], axis=1))
    advantage_blocks = advantage.reshape(blocks, seq_rows)
    coefficient_all = jnp.take_along_axis(advantage_blocks, segment, axis=1).reshape(-1) * clip_mask.astype(jnp.float32)
    weight_low = kv_weight.astype(jnp.bfloat16).reshape(D, 2 * kv_width)

    def one_block(total, index):
        start = index * tok_rows
        rows = lax.dynamic_slice_in_dim(hidden, start, tok_rows, 0)
        projected = jnp.dot(rows, weight_low, preferred_element_type=jnp.float32)
        keys_values = projected.astype(jnp.bfloat16).reshape(tok_rows, 2, heads_kv, HD)
        query_rows = lax.dynamic_slice_in_dim(queries, start, tok_rows, 0).reshape(tok_rows, heads_kv, head_ratio, HD)
        cot_rows = lax.dynamic_slice_in_dim(cotangent, start, tok_rows, 0).reshape(tok_rows, heads_kv, head_ratio, HD)
        coef_rows = lax.dynamic_slice_in_dim(coefficient_all, start, tok_rows, 0)
        seg_rows = lax.dynamic_slice_in_dim(segment, index, 1, 0)[0]
        grad_kv = learner_grads(keys_values, query_rows, cot_rows, seg_rows, coef_rows).reshape(tok_rows, 2 * kv_width)
        partial_value = jnp.einsum('tc,tk->ck', rows, grad_kv, preferred_element_type=jnp.float32)
        return (total + rounded(partial_value), None)
    total, _ = lax.scan(one_block, jnp.zeros((D, 2 * kv_width), jnp.float32), jnp.arange(blocks, dtype=jnp.int32))
    grad = total.reshape(D, 2, kv_width)
    new_moment_one = beta_one * moment_one + (1.0 - beta_one) * grad
    new_moment_two = beta_two * moment_two + (1.0 - beta_two) * grad * grad
    first_hat = new_moment_one / (1.0 - beta_one ** adam_step)
    second_hat = new_moment_two / (1.0 - beta_two ** adam_step)
    new_weight = kv_weight - learn_rate * (first_hat / (jnp.sqrt(second_hat) + adam_epsilon) + weight_decay * kv_weight)
    req_total = dec_hidden.shape[0]
    steps_here = dec_hidden.shape[1]
    capacity = kv_cache.shape[1]
    rollout_low = new_weight.astype(jnp.bfloat16).reshape(D, 2 * kv_width)
    fresh = jnp.dot(dec_hidden.reshape(req_total * steps_here, D), rollout_low, preferred_element_type=jnp.float32)
    fresh = fresh.astype(jnp.bfloat16).reshape(req_total, steps_here, 2, heads_kv, HD)
    cache = kv_cache.reshape(req_total, capacity, 2, heads_kv, HD)
    query_dec = dec_queries.reshape(req_total, steps_here, heads_kv, head_ratio, HD)
    dec_out = decode_attend(query_dec, cache, fresh, cache_len)
    return (new_weight, new_moment_one, new_moment_two, dec_out)
```

```python
import functools
import math

import jax
import jax.numpy as jnp
from jax import lax
from jax.experimental import pallas as pl
from jax.experimental.pallas import tpu as pltpu
from jax.sharding import Mesh
from jax.sharding import PartitionSpec as P

D = 5120
QH = 40
KVH = 8
HD = 128
GROUP = 16
RATIO = QH // KVH
AXES = ("x", "zh", "zl", "c", "y")
FSDP = ("x", "zh")
TENSOR = ("zl", "c")
FSDP_POOL = ("x", "zh", "y")
MESH = pl.DeviceIdType.MESH
SEMS = 112

beta_one = 0.9
beta_two = 0.999
learn_rate = 0.001
weight_decay = 0.1
adam_epsilon = 1e-08
adam_step = 10.0
variance_floor = 0.04
masked_score = -1e30
f32 = jnp.float32
bf16 = jnp.bfloat16


def rot(index, step):
    return lax.rem(index + (step + 4), 4)


def remote(src, dst, sends, recvs, k, axis, index):
    return pltpu.make_async_remote_copy(
        src_ref=src,
        dst_ref=dst,
        send_sem=sends.at[k],
        recv_sem=recvs.at[k],
        device_id={axis: index},
        device_id_type=MESH,
    )


class Gather:
    def __init__(self, axis, block, half, sends, recvs, first):
        i = lax.axis_index(axis)
        left, right, far = rot(i, -1), rot(i, 1), rot(i, 2)

        def send(ref, k, index):
            return remote(ref, ref, sends, recvs, first + k, axis, index)

        self.own = (send(block(i), 0, right), send(block(i), 1, left))
        self.near = (send(block(left), 0, right), send(block(right), 1, left))
        self.relay = (send(half(left, 0), 2, right), send(half(right, 1), 3, left))
        self.last = (send(half(far, 0), 2, right), send(half(far, 1), 3, left))

    def start(self):
        for copy in self.own:
            copy.start()

    def forward(self):
        for arrival, copy in zip(self.near, self.relay):
            arrival.wait_recv()
            copy.start()

    def finish(self):
        for arrival in self.last:
            arrival.wait_recv()

    def drain(self):
        for copy in self.own + self.relay:
            copy.wait_send()


class Reduce:
    def __init__(self, axis, half, land, sends, recvs, first):
        i = lax.axis_index(axis)
        left, right, far = rot(i, -1), rot(i, 1), rot(i, 2)
        self.half, self.land = half, land
        self.me, self.left, self.right = i, left, right

        def send(block, h, k, index):
            return remote(half(block, h), land(k), sends, recvs, first + k, axis, index)

        self.copies = (
            send(far, 0, 0, right),
            send(far, 1, 1, left),
            send(right, 1, 2, right),
            send(left, 0, 3, left),
            send(right, 0, 4, right),
            send(left, 1, 5, left),
        )

    def start(self):
        for copy in self.copies[:4]:
            copy.start()

    def forward(self):
        for k, ref in ((0, self.half(self.right, 0)), (1, self.half(self.left, 1))):
            self.copies[k].wait_recv()
            ref[...] = (ref[...].astype(f32) + self.land(k)[...].astype(f32)).astype(bf16)
            self.copies[4 + k].start()

    def finish(self, out):
        for k in (2, 3, 4, 5):
            self.copies[k].wait_recv()
        for h, (one, two) in enumerate(((4, 3), (2, 5))):
            ref = out(h)
            total = self.half(self.me, h)[...].astype(f32) + self.land(one)[...].astype(f32)
            ref[...] = (total + self.land(two)[...].astype(f32)).astype(ref.dtype)

    def drain(self):
        for copy in self.copies:
            copy.wait_send()


class GatherRows:
    def __init__(self, w, sends, recvs, first):
        x, y = lax.axis_index("x"), lax.axis_index("y")
        two = lambda h: pl.ds(2 * h, 2)
        make = lambda axis, block, half, k: Gather(axis, block, half, sends, recvs, first + 4 * k)
        self.deep = make(
            "zh", lambda j: w.at[:, x, j, y], lambda j, h: w.at[h, x, j, y], 0
        )
        self.small = (
            make("x", lambda j: w.at[0, j, :, y], lambda j, h: w.at[0, j, two(h), y], 1),
            make("y", lambda j: w.at[1, x, :, j], lambda j, h: w.at[1, x, two(h), j], 2),
        )
        self.large = (
            make("y", lambda j: w.at[0, :, :, j], lambda j, h: w.at[0, two(h), :, j], 3),
            make("x", lambda j: w.at[1, j], lambda j, h: w.at[1, j, two(h)], 4),
        )

    def drain(self):
        for part in (self.deep,) + self.small + self.large:
            part.drain()


def learner_kernel(
    hidden,
    queries,
    cotangent,
    segment,
    clip,
    rewards,
    order,
    weight,
    moment_one,
    moment_two,
    dec,
    fresh_out,
    grad_out,
    tokens,
    w,
    w_new,
    part,
    acc,
    gacc,
    q_in,
    cot_in,
    m_one,
    m_two,
    dec_in,
    stat,
    stat_land,
    land_k,
    land_v,
    sum_k,
    sum_v,
    land_k_two,
    land_v_two,
    sum_two,
    land_z,
    grads,
    local,
    sends,
    recvs,
):
    x, zh, zl, c, y = (lax.axis_index(name) for name in AXES)
    own_tokens = pltpu.make_async_copy(hidden, tokens.at[zl, c], local.at[0])
    own_tokens.start()
    q_copy = pltpu.make_async_copy(queries, q_in, local.at[1])
    q_copy.start()
    cot_copy = pltpu.make_async_copy(cotangent, cot_in, local.at[2])
    cot_copy.start()
    late = [
        pltpu.make_async_copy(src, dst, local.at[3 + k])
        for k, (src, dst) in enumerate(((moment_one, m_one), (moment_two, m_two), (dec, dec_in)))
    ]
    for copy in late:
        copy.start()

    barrier = pltpu.get_barrier_semaphore()
    peers = [("c", 1 - c)]
    for axis, index in (("zl", zl), ("zh", zh), ("x", x), ("y", y)):
        peers += [(axis, rot(index, d)) for d in (1, 2, 3)]
    for axis, index in peers:
        pl.semaphore_signal(barrier, inc=1, device_id={axis: index}, device_id_type=MESH)

    for h in range(2):
        w[h, x, zh, y] = weight[pl.ds(y * 160 + h, 80, stride=2), :].astype(bf16)
    eye = lax.broadcasted_iota(jnp.int32, (16, 16), 0) == lax.broadcasted_iota(jnp.int32, (16, 16), 1)
    reward_col = jnp.sum(jnp.where(eye, rewards[...], 0.0), axis=1, keepdims=True)
    order_col = jnp.sum(jnp.where(eye, order[...], 0), axis=1, keepdims=True)
    group_col = lax.shift_right_logical(order_col, 4)
    lane = lax.broadcasted_iota(jnp.int32, (16, 128), 1)
    member = lax.bitwise_and(lane, 63) == group_col
    reward_wide = jnp.broadcast_to(reward_col, (16, 128))
    powers = jnp.where(lane < 64, reward_wide, reward_wide * reward_wide)
    stat[0] = jnp.sum(jnp.where(member, powers, 0.0), axis=0, keepdims=True)
    own_tokens.wait()
    pl.semaphore_wait(barrier, len(peers))

    first_stat, first_rows, first_new, first_grads = 0, 9, 29, 49
    first_reduce, first_line = 53, 83
    stat_copies = []
    for k, (axis, index) in enumerate((("zh", zh), ("x", x), ("y", y))):
        stat_copies.append(
            [
                remote(stat.at[k], stat_land.at[k, d - 1], sends, recvs, first_stat + 3 * k + d - 1, axis, rot(index, d))
                for d in (1, 2, 3)
            ]
        )

    def stat_start(k):
        for copy in stat_copies[k]:
            copy.start()

    def stat_finish(k):
        for copy in stat_copies[k]:
            copy.wait_recv()
        stat[k + 1] = ((stat[k] + stat_land[k, 0]) + stat_land[k, 1]) + stat_land[k, 2]

    def shard_right(d):
        ref = tokens.at[zl - d, c]
        return remote(ref, ref, sends, recvs, first_line + d, "zl", zl + 1)

    def shard_left(d):
        ref = tokens.at[zl + d, c]
        return remote(ref, ref, sends, recvs, first_line + 3 + d, "zl", zl - 1)

    def shard_across(j, k):
        ref = tokens.at[j, c]
        return remote(ref, ref, sends, recvs, first_line + 6 + k, "c", 1 - c)

    def arrived(j, k):
        ref = tokens.at[j, c]
        remote(ref, ref, sends, recvs, first_line + k, "c", 1 - c).wait_recv()

    def crossed(j, k):
        ref = tokens.at[j, 1 - c]
        remote(ref, ref, sends, recvs, first_line + 6 + k, "c", 1 - c).wait_recv()

    rows = GatherRows(w, sends, recvs, first_rows)
    rows.deep.start()
    stat_start(0)

    @pl.when(zl < 3)
    def _():
        shard_right(0).start()

    @pl.when(zl > 0)
    def _():
        shard_left(0).start()

    shard_across(zl, 0).start()

    def pass_on(d):
        @pl.when(zl >= d)
        def _():
            arrived(zl - d, d - 1)
            if d < 3:

                @pl.when(zl < 3)
                def _():
                    shard_right(d).start()

            shard_across(zl - d, d).start()

        @pl.when(zl + d <= 3)
        def _():
            arrived(zl + d, 3 + d - 1)
            if d < 3:

                @pl.when(zl > 0)
                def _():
                    shard_left(d).start()

            shard_across(zl + d, 3 + d).start()

    rows.deep.forward()
    rows.deep.finish()
    for part_of in rows.small:
        part_of.start()
    stat_finish(0)
    stat_start(1)
    for part_of in rows.small:
        part_of.forward()
    for part_of in rows.small:
        part_of.finish()
    for part_of in rows.large:
        part_of.start()
    stat_finish(1)
    stat_start(2)
    pass_on(1)
    for part_of in rows.large:
        part_of.forward()
    for part_of in rows.large:
        part_of.finish()
    stat_finish(2)

    def rows_of(source, j, half):
        pieces = [source[h, j, pl.ds(2 * half, 2)].reshape(640, HD) for h in range(2)]
        return jnp.concatenate(pieces, axis=1)

    acc[...] = jnp.zeros_like(acc)

    def project(j):
        for half in range(2):
            acc[...] += jnp.dot(tokens[j, half], rows_of(w, j, half), preferred_element_type=f32)

    crossed(zl, 0)
    project(zl)

    def take(d):
        @pl.when(zl >= d)
        def _():
            crossed(zl - d, d)
            project(zl - d)

        @pl.when(zl + d <= 3)
        def _():
            crossed(zl + d, 3 + d)
            project(zl + d)

    pass_on(2)
    take(1)
    pass_on(3)
    take(2)
    take(3)

    sums = stat[3]
    means = sums[:, :64] / GROUP
    spreads = sums[:, 64:] / GROUP - means * means
    denoms = jnp.sqrt(jnp.maximum(spreads, variance_floor))
    in_group = lax.broadcasted_iota(jnp.int32, (16, 64), 1) == group_col
    mean_col = jnp.sum(jnp.where(in_group, means, 0.0), axis=1, keepdims=True)
    denom_col = jnp.sum(jnp.where(in_group, denoms, 0.0), axis=1, keepdims=True)
    advantage = (reward_col - mean_col) / denom_col
    block = q_in.shape[0]
    seg_row = segment[...]
    of_seq = lax.broadcasted_iota(jnp.int32, (16, block), 0) == seg_row
    coef_row = jnp.sum(jnp.where(of_seq, advantage, 0.0), axis=0, keepdims=True) * clip[...].astype(f32)
    coef_col = jnp.transpose(jnp.broadcast_to(coef_row, (HD, block)))
    seg_float = seg_row.astype(f32)
    seg_col = jnp.transpose(jnp.broadcast_to(seg_float, (HD, block)))

    scale = 1.0 / math.sqrt(HD)
    q_copy.wait()
    cot_copy.wait()
    keys = acc[:, :HD].astype(bf16)
    values = acc[:, HD:].astype(bf16)
    gacc[...] = jnp.zeros_like(gacc)
    contract_last = (((1,), (1,)), ((), ()))
    for i in range(block // HD):
        here = slice(HD * i, HD * (i + 1))
        upto = HD * (i + 1)
        heads = [slice(HD * h, HD * (h + 1)) for h in range(RATIO)]
        q_rows = jnp.concatenate([q_in[here, h] for h in heads], axis=0)
        coef_here = coef_col[here]
        up_rows = jnp.concatenate(
            [(coef_here * cot_in[here, h].astype(f32)).astype(bf16) for h in heads], axis=0
        )
        u_place = lax.broadcasted_iota(jnp.int32, (upto, HD), 0)
        t_place = lax.broadcasted_iota(jnp.int32, (upto, HD), 1) + HD * i
        allowed = (seg_col[:upto] == seg_float[:, here]) & (u_place <= t_place)
        bias = jnp.where(allowed, 0.0, masked_score)
        scores = lax.dot_general(keys[:upto], q_rows, contract_last, preferred_element_type=f32)
        scores = scores * scale + jnp.concatenate([bias] * RATIO, axis=1)
        top = jnp.max(scores, axis=0, keepdims=True)
        weights = jnp.exp(scores - top)
        attention = weights * (1.0 / jnp.sum(weights, axis=0, keepdims=True))
        grad_prob = lax.dot_general(values[:upto], up_rows, contract_last, preferred_element_type=f32)
        inner = jnp.sum(attention * grad_prob, axis=0, keepdims=True)
        grad_score = (attention * (grad_prob - inner) * scale).astype(bf16)
        gacc[:upto, :HD] += jnp.dot(grad_score, q_rows, preferred_element_type=f32)
        gacc[:upto, HD:] += jnp.dot(attention.astype(bf16), up_rows, preferred_element_type=f32)

    grad_kv = gacc[...].astype(bf16)

    def outer(j, carry):
        for half in range(2):
            product = lax.dot_general(
                tokens[j, half], grad_kv, (((0,), (0,)), ((), ())), preferred_element_type=f32
            ).astype(bf16)
            for h in range(2):
                part[h, j, pl.ds(2 * half, 2)] = product[:, HD * h : HD * (h + 1)].reshape(2, 4, 80, HD)
        return carry

    lax.fori_loop(0, 4, outer, 0)

    two = lambda h: pl.ds(2 * h, 2)
    reduce_k = Reduce(
        "y", lambda j, h: part.at[0, two(h), :, j], lambda k: land_k.at[k], sends, recvs, first_reduce
    )
    reduce_v = Reduce(
        "x", lambda j, h: part.at[1, j, two(h)], lambda k: land_v.at[k], sends, recvs, first_reduce + 6
    )
    reduce_k_two = Reduce(
        "x", lambda j, h: sum_k.at[j, two(h)], lambda k: land_k_two.at[k], sends, recvs, first_reduce + 12
    )
    reduce_v_two = Reduce(
        "y", lambda j, h: sum_v.at[two(h), j], lambda k: land_v_two.at[k], sends, recvs, first_reduce + 18
    )
    reduce_z = Reduce(
        "zh", lambda j, h: sum_two.at[h, j], lambda k: land_z.at[k], sends, recvs, first_reduce + 24
    )
    reduce_k.start()
    reduce_v.start()
    reduce_k.forward()
    reduce_v.forward()
    reduce_k.finish(lambda h: sum_k.at[two(h)])
    reduce_k_two.start()
    reduce_v.finish(lambda h: sum_v.at[two(h)])
    reduce_v_two.start()
    reduce_k_two.forward()
    reduce_v_two.forward()
    reduce_k_two.finish(lambda h: sum_two.at[0, two(h)])
    reduce_v_two.finish(lambda h: sum_two.at[1, two(h)])
    reduce_z.start()
    for copy in late:
        copy.wait()
    reduce_z.forward()
    reduce_z.finish(lambda h: grads.at[y, h])

    for h in range(2):
        quarter = pl.ds(y * 160 + h, 80, stride=2)
        grad = grads[y, h]
        one = beta_one * m_one[quarter, :] + (1.0 - beta_one) * grad
        second = beta_two * m_two[quarter, :] + (1.0 - beta_two) * grad * grad
        old = weight[quarter, :]
        new = old - learn_rate * (
            one / (1.0 - beta_one**adam_step) / (jnp.sqrt(second / (1.0 - beta_two**adam_step)) + adam_epsilon)
            + weight_decay * old
        )
        w_new[h, x, zh, y] = new.astype(bf16)
    new_rows = GatherRows(w_new, sends, recvs, first_new)
    new_rows.deep.start()
    all_grads = Gather("y", lambda j: grads.at[j], lambda j, h: grads.at[j, h], sends, recvs, first_grads)
    all_grads.start()
    new_rows.deep.forward()
    new_rows.deep.finish()
    for part_of in new_rows.small:
        part_of.start()
    all_grads.forward()
    for part_of in new_rows.small:
        part_of.forward()
    for part_of in new_rows.small:
        part_of.finish()
    for part_of in new_rows.large:
        part_of.start()
    all_grads.finish()
    grad_out[...] = grads[...]
    for part_of in new_rows.large:
        part_of.forward()
    for part_of in new_rows.large:
        part_of.finish()

    total = jnp.zeros(fresh_out.shape, f32)
    for j in range(4):
        for half in range(2):
            start = 640 * (2 * j + half)
            total += jnp.dot(dec_in[:, start : start + 640], rows_of(w_new, j, half), preferred_element_type=f32)
    fresh_out[...] = total.astype(bf16)

    for group in stat_copies:
        for copy in group:
            copy.wait_send()
    shard_across(zl, 0).wait_send()
    for d in range(3):

        @pl.when((zl >= d) & (zl < 3))
        def _():
            shard_right(d).wait_send()

        @pl.when((zl + d <= 3) & (zl > 0))
        def _():
            shard_left(d).wait_send()

    for d in (1, 2, 3):

        @pl.when(zl >= d)
        def _():
            shard_across(zl - d, d).wait_send()

        @pl.when(zl + d <= 3)
        def _():
            shard_across(zl + d, 3 + d).wait_send()

    for group in (rows, new_rows, all_grads, reduce_k, reduce_v, reduce_k_two, reduce_v_two, reduce_z):
        group.drain()


def learner(hidden, queries, cotangent, segment, clip, rewards, order, weight, moment_one, moment_two, dec):
    anywhere = pl.BlockSpec(memory_space=pl.ANY)
    vmem = pl.BlockSpec(memory_space=pltpu.VMEM)
    block, features = hidden.shape
    full = (2, 4, 4, 4, 80, HD)
    low = lambda *shape: pltpu.VMEM(shape, bf16)
    wide = lambda *shape: pltpu.VMEM(shape, f32)
    return pl.pallas_call(
        learner_kernel,
        out_shape=(
            jax.ShapeDtypeStruct((dec.shape[0], 2 * HD), bf16),
            jax.ShapeDtypeStruct((4, 2, 80, HD), f32),
        ),
        in_specs=[anywhere] * 3 + [vmem] * 5 + [anywhere] * 3,
        out_specs=(vmem, vmem),
        scratch_shapes=[
            low(4, 2, block, features),
            low(*full),
            low(*full),
            low(*full),
            wide(block, 2 * HD),
            wide(block, 2 * HD),
            low(block, features),
            low(block, features),
            wide(640, HD),
            wide(640, HD),
            low(*dec.shape),
            wide(4, 1, HD),
            wide(3, 3, 1, HD),
            low(6, 2, 4, 80, HD),
            low(6, 2, 4, 80, HD),
            low(4, 4, 80, HD),
            low(4, 4, 80, HD),
            low(6, 2, 80, HD),
            low(6, 2, 80, HD),
            low(2, 4, 80, HD),
            low(6, 80, HD),
            wide(4, 2, 80, HD),
            pltpu.SemaphoreType.DMA((6,)),
            pltpu.SemaphoreType.DMA((SEMS,)),
            pltpu.SemaphoreType.DMA((SEMS,)),
        ],
        compiler_params=pltpu.CompilerParams(collective_id=0, has_side_effects=True),
        name="learner",
    )(hidden, queries, cotangent, segment, clip, rewards, order, weight, moment_one, moment_two, dec)


def decode_attend(queries, cache, fresh, lengths):
    head_size = queries.shape[4]
    steps_here = queries.shape[1]
    capacity = cache.shape[1]
    score_scale = 1.0 / math.sqrt(head_size)
    cached = (
        jnp.einsum("bshqd,blhd->bshql", queries, cache[:, :, 0], preferred_element_type=f32)
        * score_scale
    )
    recent = (
        jnp.einsum("bshqd,bjhd->bshqj", queries, fresh[:, :, 0], preferred_element_type=f32)
        * score_scale
    )
    live = jnp.arange(capacity)[None, :] < lengths[:, None]
    cached = jnp.where(live[:, None, None, None, :], cached, masked_score)
    before = jnp.arange(steps_here)[None, :] <= jnp.arange(steps_here)[:, None]
    recent = jnp.where(before[None, :, None, None, :], recent, masked_score)
    row_max = jnp.maximum(
        jnp.max(cached, axis=-1, keepdims=True), jnp.max(recent, axis=-1, keepdims=True)
    )
    cached_exp = jnp.exp(cached - row_max)
    recent_exp = jnp.exp(recent - row_max)
    total = jnp.sum(cached_exp, axis=-1, keepdims=True) + jnp.sum(
        recent_exp, axis=-1, keepdims=True
    )
    cached_low = (cached_exp / total).astype(bf16)
    recent_low = (recent_exp / total).astype(bf16)
    output = jnp.einsum(
        "bshql,blhd->bshqd", cached_low, cache[:, :, 1], preferred_element_type=f32
    )
    output = output + jnp.einsum(
        "bshqj,bjhd->bshqd", recent_low, fresh[:, :, 1], preferred_element_type=f32
    )
    return output.astype(bf16).reshape(queries.shape[0], steps_here, -1)


def body(
    hidden,
    queries,
    cotangent,
    segment,
    clip_mask,
    rewards,
    seq_order,
    kv_weight,
    moment_one,
    moment_two,
    dec_hidden,
    dec_queries,
    kv_cache,
    cache_len,
):
    block_rows = hidden.shape[0]
    fold = lambda value: value.reshape(-1, HD)
    dec_rows, steps_here, _ = dec_hidden.shape
    fresh, grads = learner(
        hidden,
        queries,
        cotangent,
        segment,
        clip_mask.reshape(1, block_rows),
        rewards.reshape(1, -1),
        seq_order.reshape(1, -1),
        fold(kv_weight),
        fold(moment_one),
        fold(moment_two),
        dec_hidden.reshape(dec_rows * steps_here, -1),
    )
    grad = jnp.swapaxes(grads, 1, 2).reshape(kv_weight.shape)
    new_moment_one = beta_one * moment_one + (1.0 - beta_one) * grad
    new_moment_two = beta_two * moment_two + (1.0 - beta_two) * grad * grad
    first_hat = new_moment_one / (1.0 - beta_one**adam_step)
    second_hat = new_moment_two / (1.0 - beta_two**adam_step)
    new_weight = kv_weight - learn_rate * (
        first_hat / (jnp.sqrt(second_hat) + adam_epsilon) + weight_decay * kv_weight
    )
    capacity = kv_cache.shape[1]
    cache = kv_cache.reshape(dec_rows, capacity, 2, 1, HD)
    query_dec = dec_queries.reshape(dec_rows, steps_here, 1, RATIO, HD)
    fresh_low = fresh.reshape(dec_rows, steps_here, 2, 1, HD)
    dec_out = decode_attend(query_dec, cache, fresh_low, cache_len)
    return (new_weight, new_moment_one, new_moment_two, dec_out)


def solution(mesh):
    finer = Mesh(mesh.devices.reshape(4, 4, 4, 2, 4), AXES)
    in_specs = (
        P(FSDP_POOL, TENSOR),
        P(FSDP_POOL, TENSOR),
        P(FSDP_POOL, TENSOR),
        P(FSDP_POOL, None),
        P(FSDP_POOL),
        P(FSDP_POOL),
        P(FSDP_POOL),
        P(FSDP, None, TENSOR),
        P(FSDP, None, TENSOR),
        P(FSDP, None, TENSOR),
        P(FSDP_POOL, None, None),
        P(FSDP_POOL, None, TENSOR),
        P(FSDP_POOL, None, None, TENSOR),
        P(FSDP_POOL),
    )
    out_specs = (
        P(FSDP, None, TENSOR),
        P(FSDP, None, TENSOR),
        P(FSDP, None, TENSOR),
        P(FSDP_POOL, None, TENSOR),
    )
    return jax.shard_map(body, mesh=finer, in_specs=in_specs, out_specs=out_specs, check_vma=False)
```

```python
import functools
import math

import jax
import jax.numpy as jnp
from jax import lax
from jax.experimental import pallas as pl
from jax.experimental.pallas import tpu as pltpu
from jax.sharding import Mesh
from jax.sharding import PartitionSpec as P

D = 5120
QH = 40
KVH = 8
HD = 128
GROUP = 16
RATIO = QH // KVH
AXES = ("x", "zh", "zl", "c", "y")
FSDP = ("x", "zh")
TENSOR = ("zl", "c")
FSDP_POOL = ("x", "zh", "y")
MESH = pl.DeviceIdType.MESH
SEMS = 232

beta_one = 0.9
beta_two = 0.999
learn_rate = 0.001
weight_decay = 0.1
adam_epsilon = 1e-08
adam_step = 10.0
variance_floor = 0.04
masked_score = -1e30
f32 = jnp.float32
bf16 = jnp.bfloat16


def rot(index, step):
    return lax.rem(index + (step + 4), 4)


def remote(src, dst, sends, recvs, k, axis, index):
    return pltpu.make_async_remote_copy(
        src_ref=src,
        dst_ref=dst,
        send_sem=sends.at[k],
        recv_sem=recvs.at[k],
        device_id={axis: index},
        device_id_type=MESH,
    )


class Gather:
    def __init__(self, axis, block, half, sends, recvs, spot):
        i = lax.axis_index(axis)
        left, right, far = rot(i, -1), rot(i, 1), rot(i, 2)
        first = spot.take(6)

        def send(ref, k, index):
            return remote(ref, ref, sends, recvs, first + k, axis, index)

        def arrival(ref, k):
            return send(ref, k, right)

        self.own = (
            send(half(i, 0), 0, right),
            send(half(i, 1), 1, left),
            send(half(i, 1), 2, right),
            send(half(i, 0), 3, left),
        )
        self.first_half = (arrival(half(left, 0), 0), arrival(half(right, 1), 1))
        self.second_half = (arrival(half(left, 1), 2), arrival(half(right, 0), 3))
        self.relay = (send(half(left, 0), 4, right), send(half(right, 1), 5, left))
        self.from_far = (arrival(half(far, 0), 4), arrival(half(far, 1), 5))

    def start(self):
        for copy in self.own:
            copy.start()

    def forward(self):
        for got, copy in zip(self.first_half, self.relay):
            got.wait_recv()
            copy.start()

    def near(self):
        for got in self.second_half:
            got.wait_recv()

    def last(self):
        for got in self.from_far:
            got.wait_recv()

    def finish(self):
        self.near()
        self.last()

    def drain(self):
        for copy in self.own + self.relay:
            copy.wait_send()


class DirectGather:
    def __init__(self, axis, block, sends, recvs, spot):
        i = lax.axis_index(axis)
        first = spot.take(3)
        self.own = [remote(block(i), block(i), sends, recvs, first + d - 1, axis, rot(i, d)) for d in (2, 1, 3)]
        self.others = [
            remote(block(rot(i, -d)), block(rot(i, -d)), sends, recvs, first + d - 1, axis, rot(i, d))
            for d in (1, 3, 2)
        ]

    def start(self):
        for copy in self.own:
            copy.start()

    def finish(self):
        for got in self.others:
            got.wait_recv()

    def drain(self):
        for copy in self.own:
            copy.wait_send()


class DirectReduce:
    def __init__(self, axis, block, land, sends, recvs, spot):
        i = lax.axis_index(axis)
        first = spot.take(3)
        self.mine, self.land = block(i), land
        self.copies = [
            remote(block(rot(i, d)), land(d - 1), sends, recvs, first + d - 1, axis, rot(i, d)) for d in (2, 1, 3)
        ]

    def start(self):
        for copy in self.copies:
            copy.start()

    def finish(self, out):
        for copy in self.copies:
            copy.wait_recv()
        total = self.mine[...].astype(f32)
        for k in range(3):
            total = total + self.land(k)[...].astype(f32)
        out[...] = total.astype(out.dtype)

    def drain(self):
        for copy in self.copies:
            copy.wait_send()


class Spots:
    def __init__(self):
        self.free = 0

    def take(self, count):
        first = self.free
        self.free += count
        return first


class Reduce:
    def __init__(self, axis, half, land, sends, recvs, spot):
        i = lax.axis_index(axis)
        first = spot.take(6)
        left, right, far = rot(i, -1), rot(i, 1), rot(i, 2)
        self.half, self.land = half, land
        self.me, self.left, self.right = i, left, right

        def send(block, h, k, index):
            return remote(half(block, h), land(k, h), sends, recvs, first + k, axis, index)

        self.copies = (
            send(far, 0, 0, right),
            send(far, 1, 1, left),
            send(right, 1, 2, right),
            send(left, 0, 3, left),
            send(right, 0, 4, right),
            send(left, 1, 5, left),
        )

    def start_far(self):
        for copy in self.copies[:2]:
            copy.start()

    def start_near(self):
        for copy in self.copies[2:4]:
            copy.start()

    def start(self):
        self.start_far()
        self.start_near()

    def forward(self):
        for h, ref in ((0, self.half(self.right, 0)), (1, self.half(self.left, 1))):
            self.copies[h].wait_recv()
            ref[...] = (ref[...].astype(f32) + self.land(h, h)[...].astype(f32)).astype(bf16)
            self.copies[4 + h].start()

    def finish(self, out):
        for k in (2, 3, 4, 5):
            self.copies[k].wait_recv()
        for h, (one, two) in enumerate(((4, 3), (2, 5))):
            ref = out(h)
            total = self.half(self.me, h)[...].astype(f32) + self.land(one, h)[...].astype(f32)
            ref[...] = (total + self.land(two, h)[...].astype(f32)).astype(ref.dtype)

    def drain(self):
        for copy in self.copies:
            copy.wait_send()


def pair(h):
    return pl.ds(2 * h, 2)


class Both:
    def __init__(self, *parts):
        self.parts = parts

    def __getattr__(self, name):
        def run(*given):
            for k, part in enumerate(self.parts):
                getattr(part, name)(*(value[k] for value in given))

        return run


class GatherRows:
    def __init__(self, w, pieces, sends, recvs, spot):
        x, y = lax.axis_index("x"), lax.axis_index("y")
        ring = lambda axis, block, half: Gather(axis, block, half, sends, recvs, spot)
        direct = lambda axis, block: DirectGather(axis, block, sends, recvs, spot)
        self.deep = ring("zh", lambda j: w.at[:, x, j, y], lambda j, h: w.at[h, x, j, y])
        self.small, self.large = [], []
        for p in pieces:
            self.small.append(
                Both(direct("x", lambda i: w.at[0, i, p, y]), direct("y", lambda i: w.at[1, x, p, i]))
            )
            self.large.append(
                Both(
                    ring("y", lambda i: w.at[0, :, p, i], lambda i, h: w.at[0, pair(h), p, i]),
                    ring("x", lambda i: w.at[1, i, p], lambda i, h: w.at[1, i, p, pair(h)]),
                )
            )

    def drain(self):
        for part in [self.deep] + self.small + self.large:
            part.drain()


def learner_kernel(
    hidden,
    queries,
    cotangent,
    segment,
    clip,
    rewards,
    order,
    weight,
    moment_one,
    moment_two,
    dec,
    dec_queries,
    kv_cache,
    cache_len,
    weight_out,
    one_out,
    two_out,
    dec_out,
    tokens,
    w,
    w_new,
    part,
    acc,
    gacc,
    q_in,
    cot_in,
    m_one,
    m_two,
    dec_in,
    dec_wide,
    dec_cut,
    cache_in,
    dec_q,
    cached,
    top_sum,
    stat,
    stat_land,
    land_k,
    land_v,
    sum_k,
    sum_v,
    land_k_two,
    land_v_two,
    sum_two,
    land_z,
    grads,
    local,
    sends,
    recvs,
):
    x, zh, zl, c, y = (lax.axis_index(name) for name in AXES)
    own_tokens = pltpu.make_async_copy(hidden, tokens.at[zl, c], local.at[0])
    own_tokens.start()
    q_copy = pltpu.make_async_copy(queries, q_in, local.at[1])
    q_copy.start()
    cot_copy = pltpu.make_async_copy(cotangent, cot_in, local.at[2])
    cot_copy.start()
    late = [
        pltpu.make_async_copy(src, dst, local.at[3 + k])
        for k, (src, dst) in enumerate(
            ((moment_one, m_one), (moment_two, m_two), (dec, dec_in), (kv_cache, cache_in))
        )
    ]
    for copy in late:
        copy.start()

    barrier = pltpu.get_barrier_semaphore()
    peers = [("c", 1 - c)]
    for axis, index in (("zl", zl), ("zh", zh), ("x", x), ("y", y)):
        peers += [(axis, rot(index, d)) for d in ((1, -1, 2) if axis in ("x", "y") else (1, -1))]
    for axis, index in peers:
        pl.semaphore_signal(barrier, inc=1, device_id={axis: index}, device_id_type=MESH)

    for h in range(2):
        w[h, x, zh, y] = weight[pl.ds(y * 160 + h, 80, stride=2), :].astype(bf16)
    eye = lax.broadcasted_iota(jnp.int32, (16, 16), 0) == lax.broadcasted_iota(jnp.int32, (16, 16), 1)
    reward_col = jnp.sum(jnp.where(eye, rewards[...], 0.0), axis=1, keepdims=True)
    order_col = jnp.sum(jnp.where(eye, order[...], 0), axis=1, keepdims=True)
    group_col = lax.shift_right_logical(order_col, 4)
    lane = lax.broadcasted_iota(jnp.int32, (16, 128), 1)
    member = lax.bitwise_and(lane, 63) == group_col
    reward_wide = jnp.broadcast_to(reward_col, (16, 128))
    powers = jnp.where(lane < 64, reward_wide, reward_wide * reward_wide)
    stat[0] = jnp.sum(jnp.where(member, powers, 0.0), axis=0, keepdims=True)
    own_tokens.wait()
    pl.semaphore_wait(barrier, len(peers))

    spot = Spots()
    first_stat, first_line = spot.take(9), spot.take(13)
    stat_copies = []
    for k, (axis, index) in enumerate((("zh", zh), ("x", x), ("y", y))):
        stat_copies.append(
            [
                remote(src, stat_land.at[k, n], sends, recvs, first_stat + 3 * k + n, axis, rot(index, d))
                for n, (src, d) in enumerate(((stat.at[k], 1), (stat.at[k], -1), (stat_land.at[k, 0], 1)))
            ]
        )

    def stat_start(k):
        for copy in stat_copies[k][:2]:
            copy.start()

    def stat_forward(k):
        stat_copies[k][0].wait_recv()
        stat_copies[k][2].start()

    def stat_finish(k):
        for copy in stat_copies[k][1:]:
            copy.wait_recv()
        stat[k + 1] = (stat[k] + stat_land[k, 0]) + (stat_land[k, 1] + stat_land[k, 2])

    def shard_right(d):
        ref = tokens.at[zl - d, c]
        return remote(ref, ref, sends, recvs, first_line + d, "zl", zl + 1)

    def shard_left(d):
        ref = tokens.at[zl + d, c]
        return remote(ref, ref, sends, recvs, first_line + 3 + d, "zl", zl - 1)

    def shard_across(j, k):
        ref = tokens.at[j, c]
        return remote(ref, ref, sends, recvs, first_line + 6 + k, "c", 1 - c)

    def arrived(j, k):
        ref = tokens.at[j, c]
        remote(ref, ref, sends, recvs, first_line + k, "c", 1 - c).wait_recv()

    def crossed(j, k):
        ref = tokens.at[j, 1 - c]
        remote(ref, ref, sends, recvs, first_line + 6 + k, "c", 1 - c).wait_recv()

    whole = pl.ds(0, 4)
    rows = GatherRows(w, (whole,), sends, recvs, spot)
    rows.deep.start()
    stat_start(0)

    @pl.when(zl < 3)
    def _():
        shard_right(0).start()

    @pl.when(zl > 0)
    def _():
        shard_left(0).start()

    shard_across(zl, 0).start()

    def pass_on(d):
        @pl.when(zl >= d)
        def _():
            arrived(zl - d, d - 1)
            if d < 3:

                @pl.when(zl < 3)
                def _():
                    shard_right(d).start()

            shard_across(zl - d, d).start()

        @pl.when(zl + d <= 3)
        def _():
            arrived(zl + d, 3 + d - 1)
            if d < 3:

                @pl.when(zl > 0)
                def _():
                    shard_left(d).start()

            shard_across(zl + d, 3 + d).start()

    rows.deep.forward()
    stat_forward(0)
    rows.deep.finish()
    rows.small[0].start()
    stat_finish(0)
    stat_start(1)
    stat_forward(1)
    rows.small[0].finish()
    rows.large[0].start()
    stat_finish(1)
    stat_start(2)
    pass_on(1)
    rows.large[0].forward()
    stat_forward(2)
    rows.large[0].finish()
    stat_finish(2)

    def rows_of(source, j, half):
        pieces = [source[h, j, pl.ds(2 * half, 2)].reshape(640, HD) for h in range(2)]
        return jnp.concatenate(pieces, axis=1)

    acc[...] = jnp.zeros_like(acc)

    def project(j):
        for half in range(2):
            acc[...] += jnp.dot(tokens[j, half], rows_of(w, j, half), preferred_element_type=f32)

    crossed(zl, 0)
    project(zl)

    def take(d):
        @pl.when(zl >= d)
        def _():
            crossed(zl - d, d)
            project(zl - d)

        @pl.when(zl + d <= 3)
        def _():
            crossed(zl + d, 3 + d)
            project(zl + d)

    pass_on(2)
    take(1)

    for copy in late:
        copy.wait()
    requests, steps, _ = dec_q.shape[0] // (8 * RATIO), dec_in.shape[1], None
    wide_rows = 8 * RATIO
    scale = 1.0 / math.sqrt(HD)
    contract_last = (((1,), (1,)), ((), ()))
    dec_q[...] = jnp.zeros_like(dec_q)
    for r in range(requests):
        dec_wide[steps * r : steps * (r + 1), :] = dec_in[r].astype(f32)
        for h in range(RATIO):
            start = wide_rows * r + 8 * h
            dec_q[start : start + steps, :] = dec_queries[r, :, HD * h : HD * (h + 1)].astype(f32)
    for f in range(16):
        dec_cut[f] = dec_wide[:, 320 * f : 320 * (f + 1)].astype(bf16)
    place = lax.broadcasted_iota(jnp.int32, (wide_rows, cache_in.shape[1]), 1)
    for r in range(requests):
        mine = slice(wide_rows * r, wide_rows * (r + 1))
        dots = lax.dot_general(dec_q[mine, :].astype(bf16), cache_in[r], contract_last, preferred_element_type=f32)
        live = (place < 2 * cache_len[r]) & (lax.bitwise_and(place, 1) == 0)
        dots = jnp.where(live, dots * scale, masked_score)
        top = jnp.max(dots, axis=1, keepdims=True)
        powers = jnp.exp(dots - top)
        top_sum[0, mine, :] = jnp.broadcast_to(top, (wide_rows, HD))
        top_sum[1, mine, :] = jnp.broadcast_to(jnp.sum(powers, axis=1, keepdims=True), (wide_rows, HD))
        cached[r] = pltpu.roll(powers, 1, 1)

    pass_on(3)
    take(2)
    take(3)

    sums = stat[3]
    means = sums[:, :64] / GROUP
    spreads = sums[:, 64:] / GROUP - means * means
    denoms = jnp.sqrt(jnp.maximum(spreads, variance_floor))
    in_group = lax.broadcasted_iota(jnp.int32, (16, 64), 1) == group_col
    mean_col = jnp.sum(jnp.where(in_group, means, 0.0), axis=1, keepdims=True)
    denom_col = jnp.sum(jnp.where(in_group, denoms, 0.0), axis=1, keepdims=True)
    advantage = (reward_col - mean_col) / denom_col
    block = q_in.shape[0]
    seg_row = segment[...]
    of_seq = lax.broadcasted_iota(jnp.int32, (16, block), 0) == seg_row
    coef_row = jnp.sum(jnp.where(of_seq, advantage, 0.0), axis=0, keepdims=True) * clip[...].astype(f32)
    coef_col = jnp.transpose(jnp.broadcast_to(coef_row, (HD, block)))
    seg_float = seg_row.astype(f32)
    seg_col = jnp.transpose(jnp.broadcast_to(seg_float, (HD, block)))

    q_copy.wait()
    cot_copy.wait()
    keys = acc[:, :HD].astype(bf16)
    values = acc[:, HD:].astype(bf16)
    gacc[...] = jnp.zeros_like(gacc)
    for i in range(block // HD):
        here = slice(HD * i, HD * (i + 1))
        upto = HD * (i + 1)
        heads = [slice(HD * h, HD * (h + 1)) for h in range(RATIO)]
        q_rows = jnp.concatenate([q_in[here, h] for h in heads], axis=0)
        coef_here = coef_col[here]
        up_rows = jnp.concatenate(
            [(coef_here * cot_in[here, h].astype(f32)).astype(bf16) for h in heads], axis=0
        )
        u_place = lax.broadcasted_iota(jnp.int32, (upto, HD), 0)
        t_place = lax.broadcasted_iota(jnp.int32, (upto, HD), 1) + HD * i
        allowed = (seg_col[:upto] == seg_float[:, here]) & (u_place <= t_place)
        bias = jnp.where(allowed, 0.0, masked_score)
        scores = lax.dot_general(keys[:upto], q_rows, contract_last, preferred_element_type=f32)
        scores = scores * scale + jnp.concatenate([bias] * RATIO, axis=1)
        top = jnp.max(scores, axis=0, keepdims=True)
        weights = jnp.exp(scores - top)
        attention = weights * (1.0 / jnp.sum(weights, axis=0, keepdims=True))
        grad_prob = lax.dot_general(values[:upto], up_rows, contract_last, preferred_element_type=f32)
        inner = jnp.sum(attention * grad_prob, axis=0, keepdims=True)
        grad_score = (attention * (grad_prob - inner) * scale).astype(bf16)
        gacc[:upto, :HD] += jnp.dot(grad_score, q_rows, preferred_element_type=f32)
        gacc[:upto, HD:] += jnp.dot(attention.astype(bf16), up_rows, preferred_element_type=f32)

    grad_kv = gacc[...].astype(bf16)

    def outer(half):
        def step(j, carry):
            product = lax.dot_general(
                tokens[j, half], grad_kv, (((0,), (0,)), ((), ())), preferred_element_type=f32
            ).astype(bf16)
            for h in range(2):
                part[h, j, pl.ds(2 * half, 2)] = product[:, HD * h : HD * (h + 1)].reshape(2, 4, 80, HD)
            return carry

        lax.fori_loop(0, 4, step, 0)

    far = rot(zh, 2)
    near = lambda p: p + 1 - 2 * lax.rem(p, 2)
    order_of = (far, near(far), near(zh), zh)
    ring = lambda axis, half, land: Reduce(axis, half, land, sends, recvs, spot)
    direct = lambda axis, block, land: DirectReduce(axis, block, land, sends, recvs, spot)
    one, two, one_to, two_to = [], [], [], []
    for n, p in enumerate(order_of):
        one.append(
            Both(
                ring("y", lambda i, h, p=p: part.at[0, pair(h), p, i], lambda k, h, n=n: land_k.at[n, k]),
                ring("x", lambda i, h, p=p: part.at[1, i, p, pair(h)], lambda k, h, n=n: land_v.at[n, k]),
            )
        )
        one_to.append((lambda h, p=p: sum_k.at[pair(h), p], lambda h, p=p: sum_v.at[p, pair(h)]))
        two.append(
            Both(
                direct("x", lambda i, p=p: sum_k.at[i, p], lambda k, n=n: land_k_two.at[n, k]),
                direct("y", lambda i, p=p: sum_v.at[p, i], lambda k, n=n: land_v_two.at[n, k]),
            )
        )
        two_to.append((sum_two.at[0, p], sum_two.at[1, p]))
    reduce_z = ring("zh", lambda j, h: sum_two.at[h, j], lambda k, h: land_z.at[k])

    outer(lax.div(far, 2))
    one[0].start()
    outer(lax.div(zh, 2))
    one[1].start()
    one[0].forward()
    one[2].start()
    one[0].finish(one_to[0])
    two[0].start()
    one[1].forward()
    one[3].start()
    one[1].finish(one_to[1])
    two[1].start()
    two[0].finish(two_to[0])
    reduce_z.start_far()
    one[2].forward()
    one[2].finish(one_to[2])
    two[2].start()
    one[3].forward()
    two[1].finish(two_to[1])
    two[2].finish(two_to[2])
    reduce_z.start_near()
    one[3].finish(one_to[3])
    two[3].start()
    reduce_z.forward()
    two[3].finish(two_to[3])
    reduce_z.finish(lambda h: grads.at[y, h])

    def update(start, h, grad):
        rows_here = pl.ds(start + h, 80, stride=2)
        first = beta_one * m_one[rows_here, :] + (1.0 - beta_one) * grad
        second = beta_two * m_two[rows_here, :] + (1.0 - beta_two) * grad * grad
        old = weight[rows_here, :]
        first_hat = first / (1.0 - beta_one**adam_step)
        second_hat = second / (1.0 - beta_two**adam_step)
        new = old - learn_rate * (first_hat / (jnp.sqrt(second_hat) + adam_epsilon) + weight_decay * old)
        return rows_here, new, first, second

    for h in range(2):
        w_new[h, x, zh, y] = update(y * 160, h, grads[y, h])[1].astype(bf16)
    pieces = (zh, rot(zh, -1), rot(zh, 1), far)
    new_rows = GatherRows(w_new, pieces, sends, recvs, spot)
    small, large = new_rows.small, new_rows.large
    all_grads = Gather("y", lambda j: grads.at[j], lambda j, h: grads.at[j, h], sends, recvs, spot)
    fresh_total = jnp.zeros((dec_wide.shape[0], 2 * HD), f32)

    def fresh_of(p):
        added = jnp.zeros((dec_wide.shape[0], 2 * HD), f32)
        for i in range(4):
            columns = jnp.concatenate([w_new[h, i, p].reshape(320, HD) for h in range(2)], axis=1)
            added += jnp.dot(dec_cut[4 * i + p], columns, preferred_element_type=f32)
        return added

    new_rows.deep.start()
    small[0].start()
    all_grads.start()
    small[0].finish()
    large[0].start()
    all_grads.forward()
    new_rows.deep.forward()
    new_rows.deep.near()
    small[1].start()
    small[2].start()
    large[0].forward()
    small[1].finish()
    large[1].start()
    small[2].finish()
    large[2].start()
    new_rows.deep.last()
    small[3].start()
    large[0].finish()
    large[1].forward()
    small[3].finish()
    large[3].start()
    large[2].forward()
    fresh_total += fresh_of(pieces[0])
    large[1].finish()
    fresh_total += fresh_of(pieces[1])
    large[3].forward()
    large[2].finish()
    fresh_total += fresh_of(pieces[2])
    large[3].finish()
    fresh_total += fresh_of(pieces[3])

    fresh = fresh_total.astype(bf16)
    recent = lax.dot_general(dec_q[...].astype(bf16), fresh[:, :HD], contract_last, preferred_element_type=f32)
    row = lax.broadcasted_iota(jnp.int32, recent.shape, 0)
    column = lax.broadcasted_iota(jnp.int32, recent.shape, 1)
    first_row = lax.div(column, steps) * wide_rows
    seen = (row >= first_row) & (row < first_row + wide_rows)
    seen = seen & (lax.rem(column, steps) <= lax.bitwise_and(row, 7))
    recent = jnp.where(seen, recent * scale, masked_score)
    old_top = top_sum[0, :, :1]
    top = jnp.maximum(old_top, jnp.max(recent, axis=1, keepdims=True))
    shrink = jnp.exp(old_top - top)
    powers = jnp.exp(recent - top)
    total = top_sum[1, :, :1] * shrink + jnp.sum(powers, axis=1, keepdims=True)
    by_fresh = jnp.dot((powers / total).astype(bf16), fresh[:, HD:], preferred_element_type=f32)
    factor = shrink / total
    for r in range(requests):
        mine = slice(wide_rows * r, wide_rows * (r + 1))
        dec_weights = (cached[r] * factor[mine]).astype(bf16)
        result = by_fresh[mine] + jnp.dot(dec_weights, cache_in[r], preferred_element_type=f32)
        for h in range(RATIO):
            dec_out[r, :, HD * h : HD * (h + 1)] = result[8 * h : 8 * h + steps].astype(bf16)

    all_grads.finish()
    for quarter in range(4):
        for h in range(2):
            rows_here, new, first, second = update(160 * quarter, h, grads[quarter, h])
            weight_out[rows_here, :] = new
            one_out[rows_here, :] = first
            two_out[rows_here, :] = second

    for group in stat_copies:
        for copy in group:
            copy.wait_send()
    shard_across(zl, 0).wait_send()
    for d in range(3):

        @pl.when((zl >= d) & (zl < 3))
        def _():
            shard_right(d).wait_send()

        @pl.when((zl + d <= 3) & (zl > 0))
        def _():
            shard_left(d).wait_send()

    for d in (1, 2, 3):

        @pl.when(zl >= d)
        def _():
            shard_across(zl - d, d).wait_send()

        @pl.when(zl + d <= 3)
        def _():
            shard_across(zl + d, 3 + d).wait_send()

    for group in [rows, new_rows, all_grads, reduce_z] + one + two:
        group.drain()


def learner(*operands):
    hidden, dec, dec_queries, kv_cache = operands[0], operands[10], operands[11], operands[12]
    anywhere = pl.BlockSpec(memory_space=pl.ANY)
    vmem = pl.BlockSpec(memory_space=pltpu.VMEM)
    block, features = hidden.shape
    requests = dec.shape[0]
    full = (2, 4, 4, 4, 80, HD)
    low = lambda *shape: pltpu.VMEM(shape, bf16)
    wide = lambda *shape: pltpu.VMEM(shape, f32)
    return pl.pallas_call(
        learner_kernel,
        out_shape=(
            jax.ShapeDtypeStruct((640, HD), f32),
            jax.ShapeDtypeStruct((640, HD), f32),
            jax.ShapeDtypeStruct((640, HD), f32),
            jax.ShapeDtypeStruct(dec_queries.shape, bf16),
        ),
        in_specs=[anywhere] * 3 + [vmem] * 5 + [anywhere] * 3 + [vmem, anywhere, pl.BlockSpec(memory_space=pltpu.SMEM)],
        out_specs=(vmem,) * 4,
        scratch_shapes=[
            low(4, 2, block, features),
            low(*full),
            low(*full),
            low(*full),
            wide(block, 2 * HD),
            wide(block, 2 * HD),
            low(block, features),
            low(block, features),
            wide(640, HD),
            wide(640, HD),
            low(*dec.shape),
            wide(requests * dec.shape[1], dec.shape[2]),
            low(16, requests * dec.shape[1], 320),
            low(*kv_cache.shape),
            wide(requests * 8 * RATIO, HD),
            wide(requests, 8 * RATIO, kv_cache.shape[1]),
            wide(2, requests * 8 * RATIO, HD),
            wide(4, 1, HD),
            wide(3, 3, 1, HD),
            low(4, 6, 2, 80, HD),
            low(4, 6, 2, 80, HD),
            low(4, 4, 80, HD),
            low(4, 4, 80, HD),
            low(4, 3, 80, HD),
            low(4, 3, 80, HD),
            low(2, 4, 80, HD),
            low(6, 80, HD),
            wide(4, 2, 80, HD),
            pltpu.SemaphoreType.DMA((7,)),
            pltpu.SemaphoreType.DMA((SEMS,)),
            pltpu.SemaphoreType.DMA((SEMS,)),
        ],
        compiler_params=pltpu.CompilerParams(collective_id=0, has_side_effects=True),
        name="learner",
    )(*operands)


def put_kernel(*refs):
    count = (len(refs) - 1) // 2
    copies = [pltpu.make_async_copy(refs[k], refs[count + k], refs[-1].at[k]) for k in range(count)]
    for copy in copies:
        copy.start()
    for copy in copies:
        copy.wait()


def put(*arrays):
    return pl.pallas_call(
        put_kernel,
        out_shape=[jax.ShapeDtypeStruct(array.shape, array.dtype) for array in arrays],
        in_specs=[pl.BlockSpec(memory_space=pltpu.VMEM)] * len(arrays),
        out_specs=[pl.BlockSpec(memory_space=pltpu.HBM)] * len(arrays),
        scratch_shapes=[pltpu.SemaphoreType.DMA((len(arrays),))],
        name="put",
    )(*arrays)


def body(
    hidden,
    queries,
    cotangent,
    segment,
    clip_mask,
    rewards,
    seq_order,
    kv_weight,
    moment_one,
    moment_two,
    dec_hidden,
    dec_queries,
    kv_cache,
    cache_len,
):
    block_rows = hidden.shape[0]
    fold = lambda value: value.reshape(-1, HD)
    requests, capacity = kv_cache.shape[:2]
    results = learner(
        hidden,
        queries,
        cotangent,
        segment,
        clip_mask.reshape(1, block_rows),
        rewards.reshape(1, -1),
        seq_order.reshape(1, -1),
        fold(kv_weight),
        fold(moment_one),
        fold(moment_two),
        dec_hidden,
        dec_queries,
        kv_cache.reshape(requests, 2 * capacity, HD),
        cache_len,
    )
    *updated, dec_out = put(*results)
    return (*(value.reshape(kv_weight.shape) for value in updated), dec_out)


def solution(mesh):
    finer = Mesh(mesh.devices.reshape(4, 4, 4, 2, 4), AXES)
    in_specs = (
        P(FSDP_POOL, TENSOR),
        P(FSDP_POOL, TENSOR),
        P(FSDP_POOL, TENSOR),
        P(FSDP_POOL, None),
        P(FSDP_POOL),
        P(FSDP_POOL),
        P(FSDP_POOL),
        P(FSDP, None, TENSOR),
        P(FSDP, None, TENSOR),
        P(FSDP, None, TENSOR),
        P(FSDP_POOL, None, None),
        P(FSDP_POOL, None, TENSOR),
        P(FSDP_POOL, None, None, TENSOR),
        P(FSDP_POOL),
    )
    out_specs = (
        P(FSDP, None, TENSOR),
        P(FSDP, None, TENSOR),
        P(FSDP, None, TENSOR),
        P(FSDP_POOL, None, TENSOR),
    )
    return jax.shard_map(body, mesh=finer, in_specs=in_specs, out_specs=out_specs, check_vma=False)
```

```python
import functools
import math

import jax
import jax.numpy as jnp
from jax import lax
from jax.experimental import pallas as pl
from jax.experimental.pallas import tpu as pltpu
from jax.sharding import Mesh
from jax.sharding import PartitionSpec as P

D = 5120
QH = 40
KVH = 8
HD = 128
GROUP = 16
RATIO = QH // KVH
AXES = ("x", "zh", "zl", "c", "y")
FSDP = ("x", "zh")
TENSOR = ("zl", "c")
FSDP_POOL = ("x", "zh", "y")
MESH = pl.DeviceIdType.MESH
SEMS = 232

beta_one = 0.9
beta_two = 0.999
learn_rate = 0.001
weight_decay = 0.1
adam_epsilon = 1e-08
adam_step = 10.0
variance_floor = 0.04
masked_score = -1e30
f32 = jnp.float32
bf16 = jnp.bfloat16


def rot(index, step):
    return lax.rem(index + (step + 4), 4)


def remote(src, dst, sends, recvs, k, axis, index):
    return pltpu.make_async_remote_copy(
        src_ref=src,
        dst_ref=dst,
        send_sem=sends.at[k],
        recv_sem=recvs.at[k],
        device_id={axis: index},
        device_id_type=MESH,
    )


class Gather:
    def __init__(self, axis, block, half, sends, recvs, spot):
        i = lax.axis_index(axis)
        left, right, far = rot(i, -1), rot(i, 1), rot(i, 2)
        first = spot.take(6)

        def send(ref, k, index):
            return remote(ref, ref, sends, recvs, first + k, axis, index)

        def arrival(ref, k):
            return send(ref, k, right)

        self.own = (
            send(half(i, 0), 0, right),
            send(half(i, 1), 1, left),
            send(half(i, 1), 2, right),
            send(half(i, 0), 3, left),
        )
        self.first_half = (arrival(half(left, 0), 0), arrival(half(right, 1), 1))
        self.second_half = (arrival(half(left, 1), 2), arrival(half(right, 0), 3))
        self.relay = (send(half(left, 0), 4, right), send(half(right, 1), 5, left))
        self.from_far = (arrival(half(far, 0), 4), arrival(half(far, 1), 5))

    def start(self):
        for copy in self.own:
            copy.start()

    def forward(self):
        for got, copy in zip(self.first_half, self.relay):
            got.wait_recv()
            copy.start()

    def near(self):
        for got in self.second_half:
            got.wait_recv()

    def last(self):
        for got in self.from_far:
            got.wait_recv()

    def finish(self):
        self.near()
        self.last()

    def drain(self):
        for copy in self.own + self.relay:
            copy.wait_send()


class DirectGather:
    def __init__(self, axis, block, sends, recvs, spot):
        i = lax.axis_index(axis)
        first = spot.take(3)
        self.own = [remote(block(i), block(i), sends, recvs, first + d - 1, axis, rot(i, d)) for d in (2, 1, 3)]
        self.others = [
            remote(block(rot(i, -d)), block(rot(i, -d)), sends, recvs, first + d - 1, axis, rot(i, d))
            for d in (1, 3, 2)
        ]

    def start(self):
        for copy in self.own:
            copy.start()

    def finish(self):
        for got in self.others:
            got.wait_recv()

    def drain(self):
        for copy in self.own:
            copy.wait_send()


class DirectReduce:
    def __init__(self, axis, block, land, sends, recvs, spot):
        i = lax.axis_index(axis)
        first = spot.take(3)
        self.mine, self.land = block(i), land
        self.copies = [
            remote(block(rot(i, d)), land(d - 1), sends, recvs, first + d - 1, axis, rot(i, d)) for d in (2, 1, 3)
        ]

    def start(self):
        for copy in self.copies:
            copy.start()

    def finish(self, out):
        for copy in self.copies:
            copy.wait_recv()
        total = self.mine[...].astype(f32)
        for k in range(3):
            total = total + self.land(k)[...].astype(f32)
        out[...] = total.astype(out.dtype)

    def drain(self):
        for copy in self.copies:
            copy.wait_send()


class Spots:
    def __init__(self):
        self.free = 0

    def take(self, count):
        first = self.free
        self.free += count
        return first


class Reduce:
    def __init__(self, axis, half, land, sends, recvs, spot):
        i = lax.axis_index(axis)
        first = spot.take(6)
        left, right, far = rot(i, -1), rot(i, 1), rot(i, 2)
        self.half, self.land = half, land
        self.me, self.left, self.right = i, left, right

        def send(block, h, k, index):
            return remote(half(block, h), land(k, h), sends, recvs, first + k, axis, index)

        self.copies = (
            send(far, 0, 0, right),
            send(far, 1, 1, left),
            send(right, 1, 2, right),
            send(left, 0, 3, left),
            send(right, 0, 4, right),
            send(left, 1, 5, left),
        )

    def start_far(self):
        for copy in self.copies[:2]:
            copy.start()

    def start_near(self):
        for copy in self.copies[2:4]:
            copy.start()

    def start(self):
        self.start_far()
        self.start_near()

    def forward(self):
        for h, ref in ((0, self.half(self.right, 0)), (1, self.half(self.left, 1))):
            self.copies[h].wait_recv()
            ref[...] = (ref[...].astype(f32) + self.land(h, h)[...].astype(f32)).astype(bf16)
            self.copies[4 + h].start()

    def finish(self, out):
        for k in (2, 3, 4, 5):
            self.copies[k].wait_recv()
        for h, (one, two) in enumerate(((4, 3), (2, 5))):
            ref = out(h)
            total = self.half(self.me, h)[...].astype(f32) + self.land(one, h)[...].astype(f32)
            ref[...] = (total + self.land(two, h)[...].astype(f32)).astype(ref.dtype)

    def drain(self):
        for copy in self.copies:
            copy.wait_send()


def pair(h):
    return pl.ds(2 * h, 2)


class Both:
    def __init__(self, *parts):
        self.parts = parts

    def __getattr__(self, name):
        def run(*given):
            for k, part in enumerate(self.parts):
                getattr(part, name)(*(value[k] for value in given))

        return run


class GatherRows:
    def __init__(self, w, pieces, sends, recvs, spot):
        x, y = lax.axis_index("x"), lax.axis_index("y")
        ring = lambda axis, block, half: Gather(axis, block, half, sends, recvs, spot)
        direct = lambda axis, block: DirectGather(axis, block, sends, recvs, spot)
        self.deep = ring("zh", lambda j: w.at[:, x, j, y], lambda j, h: w.at[h, x, j, y])
        self.small, self.large = [], []
        for p in pieces:
            self.small.append(
                Both(direct("x", lambda i: w.at[0, i, p, y]), direct("y", lambda i: w.at[1, x, p, i]))
            )
            self.large.append(
                Both(
                    ring("y", lambda i: w.at[0, :, p, i], lambda i, h: w.at[0, pair(h), p, i]),
                    ring("x", lambda i: w.at[1, i, p], lambda i, h: w.at[1, i, p, pair(h)]),
                )
            )

    def drain(self):
        for part in [self.deep] + self.small + self.large:
            part.drain()


def learner_kernel(
    hidden,
    queries,
    cotangent,
    segment,
    clip,
    rewards,
    order,
    weight,
    moment_one,
    moment_two,
    dec,
    dec_queries,
    kv_cache,
    cache_len,
    weight_out,
    one_out,
    two_out,
    dec_out,
    tokens,
    w,
    w_new,
    part,
    acc,
    gacc,
    q_in,
    cot_in,
    m_one,
    m_two,
    dec_in,
    dec_wide,
    dec_cut,
    cache_in,
    dec_q,
    cached,
    top_sum,
    stat,
    stat_land,
    land_k,
    land_v,
    sum_k,
    sum_v,
    land_k_two,
    land_v_two,
    sum_two,
    land_z,
    grads,
    results,
    local,
    sends,
    recvs,
):
    x, zh, zl, c, y = (lax.axis_index(name) for name in AXES)
    own_tokens = pltpu.make_async_copy(hidden, tokens.at[zl, c], local.at[0])
    own_tokens.start()
    q_copy = pltpu.make_async_copy(queries, q_in, local.at[1])
    q_copy.start()
    cot_copy = pltpu.make_async_copy(cotangent, cot_in, local.at[2])
    cot_copy.start()
    late = [
        pltpu.make_async_copy(src, dst, local.at[3 + k])
        for k, (src, dst) in enumerate(
            ((moment_one, m_one), (moment_two, m_two), (dec, dec_in), (kv_cache, cache_in))
        )
    ]
    for copy in late:
        copy.start()

    barrier = pltpu.get_barrier_semaphore()
    peers = [("c", 1 - c)]
    for axis, index in (("zl", zl), ("zh", zh), ("x", x), ("y", y)):
        peers += [(axis, rot(index, d)) for d in ((1, -1, 2) if axis in ("x", "y") else (1, -1))]
    for axis, index in peers:
        pl.semaphore_signal(barrier, inc=1, device_id={axis: index}, device_id_type=MESH)

    for h in range(2):
        w[h, x, zh, y] = weight[pl.ds(y * 160 + h, 80, stride=2), :].astype(bf16)
    eye = lax.broadcasted_iota(jnp.int32, (16, 16), 0) == lax.broadcasted_iota(jnp.int32, (16, 16), 1)
    reward_col = jnp.sum(jnp.where(eye, rewards[...], 0.0), axis=1, keepdims=True)
    order_col = jnp.sum(jnp.where(eye, order[...], 0), axis=1, keepdims=True)
    group_col = lax.shift_right_logical(order_col, 4)
    lane = lax.broadcasted_iota(jnp.int32, (16, 128), 1)
    member = lax.bitwise_and(lane, 63) == group_col
    reward_wide = jnp.broadcast_to(reward_col, (16, 128))
    powers = jnp.where(lane < 64, reward_wide, reward_wide * reward_wide)
    stat[0] = jnp.sum(jnp.where(member, powers, 0.0), axis=0, keepdims=True)
    own_tokens.wait()
    pl.semaphore_wait(barrier, len(peers))

    spot = Spots()
    first_stat, first_line = spot.take(9), spot.take(26)
    stat_copies = []
    for k, (axis, index) in enumerate((("zh", zh), ("x", x), ("y", y))):
        stat_copies.append(
            [
                remote(src, stat_land.at[k, n], sends, recvs, first_stat + 3 * k + n, axis, rot(index, d))
                for n, (src, d) in enumerate(((stat.at[k], 1), (stat.at[k], -1), (stat_land.at[k, 0], 1)))
            ]
        )

    def stat_start(k):
        for copy in stat_copies[k][:2]:
            copy.start()

    def stat_forward(k):
        stat_copies[k][0].wait_recv()
        stat_copies[k][2].start()

    def stat_finish(k):
        for copy in stat_copies[k][1:]:
            copy.wait_recv()
        stat[k + 1] = (stat[k] + stat_land[k, 0]) + (stat_land[k, 1] + stat_land[k, 2])

    span = hidden.shape[0] // 2

    def half_of(j, core, q):
        return tokens.at[j, core, pl.ds(span * q, span)]

    def shard_right(d, q):
        ref = half_of(zl - d, c, q)
        return remote(ref, ref, sends, recvs, first_line + 2 * d + q, "zl", zl + 1)

    def shard_left(d, q):
        ref = half_of(zl + d, c, q)
        return remote(ref, ref, sends, recvs, first_line + 6 + 2 * d + q, "zl", zl - 1)

    def shard_across(j, k, q):
        ref = half_of(j, c, q)
        return remote(ref, ref, sends, recvs, first_line + 12 + 2 * k + q, "c", 1 - c)

    def arrived(j, k, q):
        ref = half_of(j, c, q)
        remote(ref, ref, sends, recvs, first_line + 2 * k + q, "c", 1 - c).wait_recv()

    def crossed(j, k, q):
        ref = half_of(j, 1 - c, q)
        remote(ref, ref, sends, recvs, first_line + 12 + 2 * k + q, "c", 1 - c).wait_recv()

    whole = pl.ds(0, 4)
    rows = GatherRows(w, (whole,), sends, recvs, spot)
    rows.deep.start()
    stat_start(0)

    for q in range(2):

        @pl.when(zl < 3)
        def _():
            shard_right(0, q).start()

        @pl.when(zl > 0)
        def _():
            shard_left(0, q).start()

        shard_across(zl, 0, q).start()

    def pass_on(d, q):
        @pl.when(zl >= d)
        def _():
            arrived(zl - d, d - 1, q)
            if d < 3:

                @pl.when(zl < 3)
                def _():
                    shard_right(d, q).start()

            shard_across(zl - d, d, q).start()

        @pl.when(zl + d <= 3)
        def _():
            arrived(zl + d, 3 + d - 1, q)
            if d < 3:

                @pl.when(zl > 0)
                def _():
                    shard_left(d, q).start()

            shard_across(zl + d, 3 + d, q).start()

    rows.deep.forward()
    stat_forward(0)
    pass_on(1, 0)
    rows.deep.finish()
    rows.small[0].start()
    stat_finish(0)
    stat_start(1)
    stat_forward(1)
    rows.small[0].finish()
    rows.large[0].start()
    stat_finish(1)
    stat_start(2)
    pass_on(1, 1)
    rows.large[0].forward()
    stat_forward(2)
    rows.large[0].finish()
    stat_finish(2)

    def rows_of(source, j, half):
        pieces = [source[h, j, pl.ds(2 * half, 2)].reshape(640, HD) for h in range(2)]
        return jnp.concatenate(pieces, axis=1)

    acc[...] = jnp.zeros_like(acc)

    def project(j, q):
        here = pl.ds(span * q, span)
        for half in range(2):
            acc[here, :] += jnp.dot(tokens[j, half, here], rows_of(w, j, half), preferred_element_type=f32)

    def take(d, q):
        @pl.when(zl >= d)
        def _():
            crossed(zl - d, d, q)
            project(zl - d, q)

        @pl.when(zl + d <= 3)
        def _():
            crossed(zl + d, 3 + d, q)
            project(zl + d, q)

    pass_on(2, 0)
    for q in range(2):
        crossed(zl, 0, q)
        project(zl, q)
    take(1, 0)
    take(1, 1)

    for copy in late:
        copy.wait()
    requests, steps, _ = dec_q.shape[0] // (8 * RATIO), dec_in.shape[1], None
    wide_rows = 8 * RATIO
    scale = 1.0 / math.sqrt(HD)
    contract_last = (((1,), (1,)), ((), ()))
    dec_q[...] = jnp.zeros_like(dec_q)
    for r in range(requests):
        dec_wide[steps * r : steps * (r + 1), :] = dec_in[r].astype(f32)
        for h in range(RATIO):
            start = wide_rows * r + 8 * h
            dec_q[start : start + steps, :] = dec_queries[r, :, HD * h : HD * (h + 1)].astype(f32)
    for f in range(16):
        dec_cut[f] = dec_wide[:, 320 * f : 320 * (f + 1)].astype(bf16)
    place = lax.broadcasted_iota(jnp.int32, (wide_rows, cache_in.shape[1]), 1)
    for r in range(requests):
        mine = slice(wide_rows * r, wide_rows * (r + 1))
        dots = lax.dot_general(dec_q[mine, :].astype(bf16), cache_in[r], contract_last, preferred_element_type=f32)
        live = (place < 2 * cache_len[r]) & (lax.bitwise_and(place, 1) == 0)
        dots = jnp.where(live, dots * scale, masked_score)
        top = jnp.max(dots, axis=1, keepdims=True)
        powers = jnp.exp(dots - top)
        top_sum[0, mine, :] = jnp.broadcast_to(top, (wide_rows, HD))
        top_sum[1, mine, :] = jnp.broadcast_to(jnp.sum(powers, axis=1, keepdims=True), (wide_rows, HD))
        cached[r] = pltpu.roll(powers, 1, 1)

    pass_on(2, 1)
    take(2, 0)
    take(2, 1)
    sums = stat[3]
    means = sums[:, :64] / GROUP
    spreads = sums[:, 64:] / GROUP - means * means
    denoms = jnp.sqrt(jnp.maximum(spreads, variance_floor))
    in_group = lax.broadcasted_iota(jnp.int32, (16, 64), 1) == group_col
    mean_col = jnp.sum(jnp.where(in_group, means, 0.0), axis=1, keepdims=True)
    denom_col = jnp.sum(jnp.where(in_group, denoms, 0.0), axis=1, keepdims=True)
    advantage = (reward_col - mean_col) / denom_col
    block = q_in.shape[0]
    seg_row = segment[...]
    of_seq = lax.broadcasted_iota(jnp.int32, (16, block), 0) == seg_row
    coef_row = jnp.sum(jnp.where(of_seq, advantage, 0.0), axis=0, keepdims=True) * clip[...].astype(f32)
    coef_col = jnp.transpose(jnp.broadcast_to(coef_row, (HD, block)))
    seg_float = seg_row.astype(f32)
    seg_col = jnp.transpose(jnp.broadcast_to(seg_float, (HD, block)))

    q_copy.wait()
    cot_copy.wait()
    gacc[...] = jnp.zeros_like(gacc)

    def attend(i):
        here = slice(HD * i, HD * (i + 1))
        upto = HD * (i + 1)
        keys, values = acc[:upto, :HD].astype(bf16), acc[:upto, HD:].astype(bf16)
        heads = [slice(HD * h, HD * (h + 1)) for h in range(RATIO)]
        q_rows = jnp.concatenate([q_in[here, h] for h in heads], axis=0)
        coef_here = coef_col[here]
        up_rows = jnp.concatenate(
            [(coef_here * cot_in[here, h].astype(f32)).astype(bf16) for h in heads], axis=0
        )
        u_place = lax.broadcasted_iota(jnp.int32, (upto, HD), 0)
        t_place = lax.broadcasted_iota(jnp.int32, (upto, HD), 1) + HD * i
        allowed = (seg_col[:upto] == seg_float[:, here]) & (u_place <= t_place)
        bias = jnp.where(allowed, 0.0, masked_score)
        scores = lax.dot_general(keys, q_rows, contract_last, preferred_element_type=f32)
        scores = scores * scale + jnp.concatenate([bias] * RATIO, axis=1)
        top = jnp.max(scores, axis=0, keepdims=True)
        weights = jnp.exp(scores - top)
        attention = weights * (1.0 / jnp.sum(weights, axis=0, keepdims=True))
        grad_prob = lax.dot_general(values, up_rows, contract_last, preferred_element_type=f32)
        inner = jnp.sum(attention * grad_prob, axis=0, keepdims=True)
        grad_score = (attention * (grad_prob - inner) * scale).astype(bf16)
        gacc[:upto, :HD] += jnp.dot(grad_score, q_rows, preferred_element_type=f32)
        gacc[:upto, HD:] += jnp.dot(attention.astype(bf16), up_rows, preferred_element_type=f32)

    for q in range(2):
        pass_on(3, q)
        take(3, q)
        attend(2 * q)
        attend(2 * q + 1)

    grad_kv = gacc[...].astype(bf16)

    def outer(half):
        def step(j, carry):
            product = lax.dot_general(
                tokens[j, half], grad_kv, (((0,), (0,)), ((), ())), preferred_element_type=f32
            ).astype(bf16)
            for h in range(2):
                part[h, j, pl.ds(2 * half, 2)] = product[:, HD * h : HD * (h + 1)].reshape(2, 4, 80, HD)
            return carry

        lax.fori_loop(0, 4, step, 0)

    far = rot(zh, 2)
    near = lambda p: p + 1 - 2 * lax.rem(p, 2)
    order_of = (far, near(far), near(zh), zh)
    ring = lambda axis, half, land: Reduce(axis, half, land, sends, recvs, spot)
    direct = lambda axis, block, land: DirectReduce(axis, block, land, sends, recvs, spot)
    one, two, one_to, two_to = [], [], [], []
    for n, p in enumerate(order_of):
        one.append(
            Both(
                ring("y", lambda i, h, p=p: part.at[0, pair(h), p, i], lambda k, h, n=n: land_k.at[n, k]),
                ring("x", lambda i, h, p=p: part.at[1, i, p, pair(h)], lambda k, h, n=n: land_v.at[n, k]),
            )
        )
        one_to.append((lambda h, p=p: sum_k.at[pair(h), p], lambda h, p=p: sum_v.at[p, pair(h)]))
        two.append(
            Both(
                direct("x", lambda i, p=p: sum_k.at[i, p], lambda k, n=n: land_k_two.at[n, k]),
                direct("y", lambda i, p=p: sum_v.at[p, i], lambda k, n=n: land_v_two.at[n, k]),
            )
        )
        two_to.append((sum_two.at[0, p], sum_two.at[1, p]))
    reduce_z = ring("zh", lambda j, h: sum_two.at[h, j], lambda k, h: land_z.at[k])

    outer(lax.div(far, 2))
    one[0].start()
    outer(lax.div(zh, 2))
    one[1].start()
    one[0].forward()
    one[2].start()
    one[0].finish(one_to[0])
    two[0].start()
    one[1].forward()
    one[3].start()
    one[1].finish(one_to[1])
    two[1].start()
    two[0].finish(two_to[0])
    reduce_z.start_far()
    one[2].forward()
    one[2].finish(one_to[2])
    two[2].start()
    one[3].forward()
    two[1].finish(two_to[1])
    two[2].finish(two_to[2])
    reduce_z.start_near()
    one[3].finish(one_to[3])
    two[3].start()
    reduce_z.forward()
    two[3].finish(two_to[3])
    reduce_z.finish(lambda h: grads.at[y, h])

    def update(start, h, grad):
        rows_here = pl.ds(start + h, 80, stride=2)
        first = beta_one * m_one[rows_here, :] + (1.0 - beta_one) * grad
        second = beta_two * m_two[rows_here, :] + (1.0 - beta_two) * grad * grad
        old = weight[rows_here, :]
        first_hat = first / (1.0 - beta_one**adam_step)
        second_hat = second / (1.0 - beta_two**adam_step)
        new = old - learn_rate * (first_hat / (jnp.sqrt(second_hat) + adam_epsilon) + weight_decay * old)
        return rows_here, new, first, second

    for h in range(2):
        w_new[h, x, zh, y] = update(y * 160, h, grads[y, h])[1].astype(bf16)
    pieces = (zh, rot(zh, -1), rot(zh, 1), far)
    new_rows = GatherRows(w_new, pieces, sends, recvs, spot)
    small, large = new_rows.small, new_rows.large
    all_grads = Gather("y", lambda j: grads.at[j], lambda j, h: grads.at[j, h], sends, recvs, spot)
    fresh_total = jnp.zeros((dec_wide.shape[0], 2 * HD), f32)

    def fresh_of(p):
        added = jnp.zeros((dec_wide.shape[0], 2 * HD), f32)
        for i in range(4):
            columns = jnp.concatenate([w_new[h, i, p].reshape(320, HD) for h in range(2)], axis=1)
            added += jnp.dot(dec_cut[4 * i + p], columns, preferred_element_type=f32)
        return added

    new_rows.deep.start()
    small[0].start()
    all_grads.start()
    small[0].finish()
    large[0].start()
    all_grads.forward()
    new_rows.deep.forward()
    new_rows.deep.near()
    small[1].start()
    small[2].start()
    large[0].forward()
    small[1].finish()
    large[1].start()
    small[2].finish()
    large[2].start()
    all_grads.finish()
    for quarter in range(4):
        for h in range(2):
            rows_here, new, first, second = update(160 * quarter, h, grads[quarter, h])
            results[0, rows_here, :] = new
            results[1, rows_here, :] = first
            results[2, rows_here, :] = second
    outs = [
        pltpu.make_async_copy(results.at[k], ref, local.at[7 + k])
        for k, ref in enumerate((weight_out, one_out, two_out))
    ]
    for copy in outs:
        copy.start()
    new_rows.deep.last()
    small[3].start()
    large[0].finish()
    large[1].forward()
    small[3].finish()
    large[3].start()
    large[2].forward()
    fresh_total += fresh_of(pieces[0])
    large[1].finish()
    fresh_total += fresh_of(pieces[1])
    large[3].forward()
    large[2].finish()
    fresh_total += fresh_of(pieces[2])
    large[3].finish()
    fresh_total += fresh_of(pieces[3])

    fresh = fresh_total.astype(bf16)
    recent = lax.dot_general(dec_q[...].astype(bf16), fresh[:, :HD], contract_last, preferred_element_type=f32)
    row = lax.broadcasted_iota(jnp.int32, recent.shape, 0)
    column = lax.broadcasted_iota(jnp.int32, recent.shape, 1)
    first_row = lax.div(column, steps) * wide_rows
    seen = (row >= first_row) & (row < first_row + wide_rows)
    seen = seen & (lax.rem(column, steps) <= lax.bitwise_and(row, 7))
    recent = jnp.where(seen, recent * scale, masked_score)
    old_top = top_sum[0, :, :1]
    top = jnp.maximum(old_top, jnp.max(recent, axis=1, keepdims=True))
    shrink = jnp.exp(old_top - top)
    powers = jnp.exp(recent - top)
    total = top_sum[1, :, :1] * shrink + jnp.sum(powers, axis=1, keepdims=True)
    by_fresh = jnp.dot((powers / total).astype(bf16), fresh[:, HD:], preferred_element_type=f32)
    factor = shrink / total
    for r in range(requests):
        mine = slice(wide_rows * r, wide_rows * (r + 1))
        dec_weights = (cached[r] * factor[mine]).astype(bf16)
        result = by_fresh[mine] + jnp.dot(dec_weights, cache_in[r], preferred_element_type=f32)
        for h in range(RATIO):
            dec_out[r, :, HD * h : HD * (h + 1)] = result[8 * h : 8 * h + steps].astype(bf16)

    for copy in outs:
        copy.wait()
    for group in stat_copies:
        for copy in group:
            copy.wait_send()
    for q in range(2):
        shard_across(zl, 0, q).wait_send()
        for d in range(3):

            @pl.when((zl >= d) & (zl < 3))
            def _():
                shard_right(d, q).wait_send()

            @pl.when((zl + d <= 3) & (zl > 0))
            def _():
                shard_left(d, q).wait_send()

        for d in (1, 2, 3):

            @pl.when(zl >= d)
            def _():
                shard_across(zl - d, d, q).wait_send()

            @pl.when(zl + d <= 3)
            def _():
                shard_across(zl + d, 3 + d, q).wait_send()

    for group in [rows, new_rows, all_grads, reduce_z] + one + two:
        group.drain()


def learner(*operands):
    hidden, dec, dec_queries, kv_cache = operands[0], operands[10], operands[11], operands[12]
    anywhere = pl.BlockSpec(memory_space=pl.ANY)
    vmem = pl.BlockSpec(memory_space=pltpu.VMEM)
    block, features = hidden.shape
    requests = dec.shape[0]
    full = (2, 4, 4, 4, 80, HD)
    low = lambda *shape: pltpu.VMEM(shape, bf16)
    wide = lambda *shape: pltpu.VMEM(shape, f32)
    return pl.pallas_call(
        learner_kernel,
        out_shape=(
            jax.ShapeDtypeStruct((640, HD), f32),
            jax.ShapeDtypeStruct((640, HD), f32),
            jax.ShapeDtypeStruct((640, HD), f32),
            jax.ShapeDtypeStruct(dec_queries.shape, bf16),
        ),
        in_specs=[anywhere] * 3 + [vmem] * 5 + [anywhere] * 3 + [vmem, anywhere, pl.BlockSpec(memory_space=pltpu.SMEM)],
        out_specs=(anywhere,) * 3 + (vmem,),
        scratch_shapes=[
            low(4, 2, block, features),
            low(*full),
            low(*full),
            low(*full),
            wide(block, 2 * HD),
            wide(block, 2 * HD),
            low(block, features),
            low(block, features),
            wide(640, HD),
            wide(640, HD),
            low(*dec.shape),
            wide(requests * dec.shape[1], dec.shape[2]),
            low(16, requests * dec.shape[1], 320),
            low(*kv_cache.shape),
            wide(requests * 8 * RATIO, HD),
            wide(requests, 8 * RATIO, kv_cache.shape[1]),
            wide(2, requests * 8 * RATIO, HD),
            wide(4, 1, HD),
            wide(3, 3, 1, HD),
            low(4, 6, 2, 80, HD),
            low(4, 6, 2, 80, HD),
            low(4, 4, 80, HD),
            low(4, 4, 80, HD),
            low(4, 3, 80, HD),
            low(4, 3, 80, HD),
            low(2, 4, 80, HD),
            low(6, 80, HD),
            wide(4, 2, 80, HD),
            wide(3, 640, HD),
            pltpu.SemaphoreType.DMA((10,)),
            pltpu.SemaphoreType.DMA((SEMS,)),
            pltpu.SemaphoreType.DMA((SEMS,)),
        ],
        compiler_params=pltpu.CompilerParams(collective_id=0, has_side_effects=True),
        name="learner",
    )(*operands)


def put_kernel(*refs):
    count = (len(refs) - 1) // 2
    copies = [pltpu.make_async_copy(refs[k], refs[count + k], refs[-1].at[k]) for k in range(count)]
    for copy in copies:
        copy.start()
    for copy in copies:
        copy.wait()


def put(*arrays):
    return pl.pallas_call(
        put_kernel,
        out_shape=[jax.ShapeDtypeStruct(array.shape, array.dtype) for array in arrays],
        in_specs=[pl.BlockSpec(memory_space=pltpu.VMEM)] * len(arrays),
        out_specs=[pl.BlockSpec(memory_space=pltpu.HBM)] * len(arrays),
        scratch_shapes=[pltpu.SemaphoreType.DMA((len(arrays),))],
        name="put",
    )(*arrays)


def body(
    hidden,
    queries,
    cotangent,
    segment,
    clip_mask,
    rewards,
    seq_order,
    kv_weight,
    moment_one,
    moment_two,
    dec_hidden,
    dec_queries,
    kv_cache,
    cache_len,
):
    block_rows = hidden.shape[0]
    fold = lambda value: value.reshape(-1, HD)
    requests, capacity = kv_cache.shape[:2]
    results = learner(
        hidden,
        queries,
        cotangent,
        segment,
        clip_mask.reshape(1, block_rows),
        rewards.reshape(1, -1),
        seq_order.reshape(1, -1),
        fold(kv_weight),
        fold(moment_one),
        fold(moment_two),
        dec_hidden,
        dec_queries,
        kv_cache.reshape(requests, 2 * capacity, HD),
        cache_len,
    )
    *updated, dec_out = put(*results)
    return (*(value.reshape(kv_weight.shape) for value in updated), dec_out)


def solution(mesh):
    finer = Mesh(mesh.devices.reshape(4, 4, 4, 2, 4), AXES)
    in_specs = (
        P(FSDP_POOL, TENSOR),
        P(FSDP_POOL, TENSOR),
        P(FSDP_POOL, TENSOR),
        P(FSDP_POOL, None),
        P(FSDP_POOL),
        P(FSDP_POOL),
        P(FSDP_POOL),
        P(FSDP, None, TENSOR),
        P(FSDP, None, TENSOR),
        P(FSDP, None, TENSOR),
        P(FSDP_POOL, None, None),
        P(FSDP_POOL, None, TENSOR),
        P(FSDP_POOL, None, None, TENSOR),
        P(FSDP_POOL),
    )
    out_specs = (
        P(FSDP, None, TENSOR),
        P(FSDP, None, TENSOR),
        P(FSDP, None, TENSOR),
        P(FSDP_POOL, None, TENSOR),
    )
    return jax.shard_map(body, mesh=finer, in_specs=in_specs, out_specs=out_specs, check_vma=False)
```

```python
import functools
import math

import jax
import jax.numpy as jnp
from jax import lax
from jax.experimental import pallas as pl
from jax.experimental.pallas import tpu as pltpu
from jax.sharding import Mesh
from jax.sharding import PartitionSpec as P

D = 5120
QH = 40
KVH = 8
HD = 128
GROUP = 16
RATIO = QH // KVH
AXES = ("x", "zh", "zl", "c", "y")
FSDP = ("x", "zh")
TENSOR = ("zl", "c")
FSDP_POOL = ("x", "zh", "y")
MESH = pl.DeviceIdType.MESH
SEMS = 256
CUTS = 4

beta_one = 0.9
beta_two = 0.999
learn_rate = 0.001
weight_decay = 0.1
adam_epsilon = 1e-08
adam_step = 10.0
variance_floor = 0.04
masked_score = -1e30
f32 = jnp.float32
bf16 = jnp.bfloat16


def rot(index, step):
    return lax.rem(index + (step + 4), 4)


def remote(src, dst, sends, recvs, k, axis, index):
    return pltpu.make_async_remote_copy(
        src_ref=src,
        dst_ref=dst,
        send_sem=sends.at[k],
        recv_sem=recvs.at[k],
        device_id={axis: index},
        device_id_type=MESH,
    )


class Gather:
    def __init__(self, axis, block, half, sends, recvs, spot):
        i = lax.axis_index(axis)
        left, right, far = rot(i, -1), rot(i, 1), rot(i, 2)
        first = spot.take(6)

        def send(ref, k, index):
            return remote(ref, ref, sends, recvs, first + k, axis, index)

        def arrival(ref, k):
            return send(ref, k, right)

        self.own = (
            send(half(i, 0), 0, right),
            send(half(i, 1), 1, left),
            send(half(i, 1), 2, right),
            send(half(i, 0), 3, left),
        )
        self.first_half = (arrival(half(left, 0), 0), arrival(half(right, 1), 1))
        self.second_half = (arrival(half(left, 1), 2), arrival(half(right, 0), 3))
        self.relay = (send(half(left, 0), 4, right), send(half(right, 1), 5, left))
        self.from_far = (arrival(half(far, 0), 4), arrival(half(far, 1), 5))

    def start(self):
        for copy in self.own:
            copy.start()

    def forward(self):
        for got, copy in zip(self.first_half, self.relay):
            got.wait_recv()
            copy.start()

    def near(self):
        for got in self.second_half:
            got.wait_recv()

    def last(self):
        for got in self.from_far:
            got.wait_recv()

    def finish(self):
        self.near()
        self.last()

    def drain(self):
        for copy in self.own + self.relay:
            copy.wait_send()


class DirectGather:
    def __init__(self, axis, block, sends, recvs, spot):
        i = lax.axis_index(axis)
        first = spot.take(3)
        self.own = [remote(block(i), block(i), sends, recvs, first + d - 1, axis, rot(i, d)) for d in (2, 1, 3)]
        self.others = [
            remote(block(rot(i, -d)), block(rot(i, -d)), sends, recvs, first + d - 1, axis, rot(i, d))
            for d in (1, 3, 2)
        ]

    def start(self):
        for copy in self.own:
            copy.start()

    def finish(self):
        for got in self.others:
            got.wait_recv()

    def drain(self):
        for copy in self.own:
            copy.wait_send()


class DirectReduce:
    def __init__(self, axis, block, land, sends, recvs, spot):
        i = lax.axis_index(axis)
        first = spot.take(3)
        self.mine, self.land = block(i), land
        self.copies = [
            remote(block(rot(i, d)), land(d - 1), sends, recvs, first + d - 1, axis, rot(i, d)) for d in (2, 1, 3)
        ]

    def start(self):
        for copy in self.copies:
            copy.start()

    def finish(self, out):
        for copy in self.copies:
            copy.wait_recv()
        total = self.mine[...].astype(f32)
        for k in range(3):
            total = total + self.land(k)[...].astype(f32)
        out[...] = total.astype(out.dtype)

    def drain(self):
        for copy in self.copies:
            copy.wait_send()


class Spots:
    def __init__(self):
        self.free = 0

    def take(self, count):
        first = self.free
        self.free += count
        return first


class Reduce:
    def __init__(self, axis, half, land, sends, recvs, spot):
        i = lax.axis_index(axis)
        first = spot.take(6)
        left, right, far = rot(i, -1), rot(i, 1), rot(i, 2)
        self.half, self.land = half, land
        self.me, self.left, self.right = i, left, right

        def send(block, h, k, index):
            return remote(half(block, h), land(k, h), sends, recvs, first + k, axis, index)

        self.copies = (
            send(far, 0, 0, right),
            send(far, 1, 1, left),
            send(right, 1, 2, right),
            send(left, 0, 3, left),
            send(right, 0, 4, right),
            send(left, 1, 5, left),
        )

    def start_far(self):
        for copy in self.copies[:2]:
            copy.start()

    def start_near(self):
        for copy in self.copies[2:4]:
            copy.start()

    def start(self):
        self.start_far()
        self.start_near()

    def forward(self):
        for h, ref in ((0, self.half(self.right, 0)), (1, self.half(self.left, 1))):
            self.copies[h].wait_recv()
            ref[...] = (ref[...].astype(f32) + self.land(h, h)[...].astype(f32)).astype(bf16)
            self.copies[4 + h].start()

    def finish(self, out):
        for k in (2, 3, 4, 5):
            self.copies[k].wait_recv()
        for h, (one, two) in enumerate(((4, 3), (2, 5))):
            ref = out(h)
            total = self.half(self.me, h)[...].astype(f32) + self.land(one, h)[...].astype(f32)
            ref[...] = (total + self.land(two, h)[...].astype(f32)).astype(ref.dtype)

    def drain(self):
        for copy in self.copies:
            copy.wait_send()


def pair(h):
    return pl.ds(2 * h, 2)


class Both:
    def __init__(self, *parts):
        self.parts = parts

    def __getattr__(self, name):
        def run(*given):
            for k, part in enumerate(self.parts):
                getattr(part, name)(*(value[k] for value in given))

        return run


class GatherRows:
    def __init__(self, w, pieces, sends, recvs, spot):
        x, y = lax.axis_index("x"), lax.axis_index("y")
        ring = lambda axis, block, half: Gather(axis, block, half, sends, recvs, spot)
        direct = lambda axis, block: DirectGather(axis, block, sends, recvs, spot)
        self.deep = ring("zh", lambda j: w.at[:, x, j, y], lambda j, h: w.at[h, x, j, y])
        self.small, self.large = [], []
        for p in pieces:
            self.small.append(
                Both(direct("x", lambda i: w.at[0, i, p, y]), direct("y", lambda i: w.at[1, x, p, i]))
            )
            self.large.append(
                Both(
                    ring("y", lambda i: w.at[0, :, p, i], lambda i, h: w.at[0, pair(h), p, i]),
                    ring("x", lambda i: w.at[1, i, p], lambda i, h: w.at[1, i, p, pair(h)]),
                )
            )

    def drain(self):
        for part in [self.deep] + self.small + self.large:
            part.drain()


def learner_kernel(
    hidden,
    queries,
    cotangent,
    segment,
    clip,
    rewards,
    order,
    weight,
    moment_one,
    moment_two,
    dec,
    dec_queries,
    kv_cache,
    cache_len,
    weight_out,
    one_out,
    two_out,
    dec_out,
    tokens,
    w,
    w_new,
    part,
    acc,
    gacc,
    q_in,
    cot_in,
    m_one,
    m_two,
    dec_in,
    dec_wide,
    dec_cut,
    cache_in,
    dec_q,
    cached,
    top_sum,
    stat,
    stat_land,
    land_k,
    land_v,
    sum_k,
    sum_v,
    land_k_two,
    land_v_two,
    sum_two,
    land_z,
    grads,
    results,
    local,
    sends,
    recvs,
):
    x, zh, zl, c, y = (lax.axis_index(name) for name in AXES)
    own_tokens = pltpu.make_async_copy(hidden, tokens.at[zl, c], local.at[0])
    own_tokens.start()
    q_copy = pltpu.make_async_copy(queries, q_in, local.at[1])
    q_copy.start()
    cot_copy = pltpu.make_async_copy(cotangent, cot_in, local.at[2])
    cot_copy.start()
    late = [
        pltpu.make_async_copy(src, dst, local.at[3 + k])
        for k, (src, dst) in enumerate(
            ((moment_one, m_one), (moment_two, m_two), (dec, dec_in), (kv_cache, cache_in))
        )
    ]
    for copy in late:
        copy.start()

    barrier = pltpu.get_barrier_semaphore()
    peers = [("c", 1 - c)]
    for axis, index in (("zl", zl), ("zh", zh), ("x", x), ("y", y)):
        peers += [(axis, rot(index, d)) for d in ((1, -1, 2) if axis in ("x", "y") else (1, -1))]
    for axis, index in peers:
        pl.semaphore_signal(barrier, inc=1, device_id={axis: index}, device_id_type=MESH)

    for h in range(2):
        w[h, x, zh, y] = weight[pl.ds(y * 160 + h, 80, stride=2), :].astype(bf16)
    eye = lax.broadcasted_iota(jnp.int32, (16, 16), 0) == lax.broadcasted_iota(jnp.int32, (16, 16), 1)
    reward_col = jnp.sum(jnp.where(eye, rewards[...], 0.0), axis=1, keepdims=True)
    order_col = jnp.sum(jnp.where(eye, order[...], 0), axis=1, keepdims=True)
    group_col = lax.shift_right_logical(order_col, 4)
    lane = lax.broadcasted_iota(jnp.int32, (16, 128), 1)
    member = lax.bitwise_and(lane, 63) == group_col
    reward_wide = jnp.broadcast_to(reward_col, (16, 128))
    powers = jnp.where(lane < 64, reward_wide, reward_wide * reward_wide)
    stat[0] = jnp.sum(jnp.where(member, powers, 0.0), axis=0, keepdims=True)
    own_tokens.wait()
    pl.semaphore_wait(barrier, len(peers))

    spot = Spots()
    first_stat, first_line = spot.take(9), spot.take(13 * CUTS)
    stat_copies = []
    for k, (axis, index) in enumerate((("zh", zh), ("x", x), ("y", y))):
        stat_copies.append(
            [
                remote(src, stat_land.at[k, n], sends, recvs, first_stat + 3 * k + n, axis, rot(index, d))
                for n, (src, d) in enumerate(((stat.at[k], 1), (stat.at[k], -1), (stat_land.at[k, 0], 1)))
            ]
        )

    def stat_start(k):
        for copy in stat_copies[k][:2]:
            copy.start()

    def stat_forward(k):
        stat_copies[k][0].wait_recv()
        stat_copies[k][2].start()

    def stat_finish(k):
        for copy in stat_copies[k][1:]:
            copy.wait_recv()
        stat[k + 1] = (stat[k] + stat_land[k, 0]) + (stat_land[k, 1] + stat_land[k, 2])

    span = hidden.shape[0] // CUTS

    def cut_of(j, core, q):
        return tokens.at[j, core, pl.ds(span * q, span)]

    def shard_right(d, q):
        ref = cut_of(zl - d, c, q)
        return remote(ref, ref, sends, recvs, first_line + CUTS * d + q, "zl", zl + 1)

    def shard_left(d, q):
        ref = cut_of(zl + d, c, q)
        return remote(ref, ref, sends, recvs, first_line + CUTS * (3 + d) + q, "zl", zl - 1)

    def shard_across(j, k, q):
        ref = cut_of(j, c, q)
        return remote(ref, ref, sends, recvs, first_line + CUTS * (6 + k) + q, "c", 1 - c)

    def arrived(j, k, q):
        ref = cut_of(j, c, q)
        remote(ref, ref, sends, recvs, first_line + CUTS * k + q, "c", 1 - c).wait_recv()

    def crossed(j, k, q):
        ref = cut_of(j, 1 - c, q)
        remote(ref, ref, sends, recvs, first_line + CUTS * (6 + k) + q, "c", 1 - c).wait_recv()

    whole = pl.ds(0, 4)
    rows = GatherRows(w, (whole,), sends, recvs, spot)
    rows.deep.start()
    stat_start(0)

    for q in range(CUTS):

        @pl.when(zl < 3)
        def _():
            shard_right(0, q).start()

        @pl.when(zl > 0)
        def _():
            shard_left(0, q).start()

    def pass_on(d, q):
        @pl.when(zl >= d)
        def _():
            arrived(zl - d, d - 1, q)
            if d < 3:

                @pl.when(zl < 3)
                def _():
                    shard_right(d, q).start()

        @pl.when(zl + d <= 3)
        def _():
            arrived(zl + d, 3 + d - 1, q)
            if d < 3:

                @pl.when(zl > 0)
                def _():
                    shard_left(d, q).start()

    def hand_over(d, q):
        @pl.when(zl >= d)
        def _():
            shard_across(zl - d, d, q).start()

        @pl.when(zl + d <= 3)
        def _():
            shard_across(zl + d, 3 + d, q).start()

    rows.deep.forward()
    stat_forward(0)
    pass_on(1, 0)
    pass_on(1, 1)
    rows.deep.finish()
    rows.small[0].start()
    stat_finish(0)
    stat_start(1)
    stat_forward(1)
    pass_on(1, 2)
    rows.small[0].finish()
    rows.large[0].start()
    stat_finish(1)
    stat_start(2)
    pass_on(1, 3)

    for q in range(CUTS):
        shard_across(zl, 0, q).start()
        hand_over(1, q)
    rows.large[0].forward()
    stat_forward(2)
    rows.large[0].finish()
    stat_finish(2)
    for q in range(CUTS):
        pass_on(2, q)
        hand_over(2, q)

    def rows_of(source, j, half):
        pieces = [source[h, j, pl.ds(2 * half, 2)].reshape(640, HD) for h in range(2)]
        return jnp.concatenate(pieces, axis=1)

    acc[...] = jnp.zeros_like(acc)

    def project(j, here):
        for half in range(2):
            acc[here, :] += jnp.dot(tokens[j, half, here], rows_of(w, j, half), preferred_element_type=f32)

    everything = pl.ds(0, hidden.shape[0])

    def take(d):
        @pl.when(zl >= d)
        def _():
            for q in range(CUTS):
                crossed(zl - d, d, q)
            project(zl - d, everything)

        @pl.when(zl + d <= 3)
        def _():
            for q in range(CUTS):
                crossed(zl + d, 3 + d, q)
            project(zl + d, everything)

    for copy in late:
        copy.wait()
    requests, steps, _ = dec_q.shape[0] // (8 * RATIO), dec_in.shape[1], None
    wide_rows = 8 * RATIO
    scale = 1.0 / math.sqrt(HD)
    contract_last = (((1,), (1,)), ((), ()))
    dec_q[...] = jnp.zeros_like(dec_q)
    for r in range(requests):
        dec_wide[steps * r : steps * (r + 1), :] = dec_in[r].astype(f32)
        for h in range(RATIO):
            start = wide_rows * r + 8 * h
            dec_q[start : start + steps, :] = dec_queries[r, :, HD * h : HD * (h + 1)].astype(f32)
    for f in range(16):
        dec_cut[f] = dec_wide[:, 320 * f : 320 * (f + 1)].astype(bf16)
    place = lax.broadcasted_iota(jnp.int32, (wide_rows, cache_in.shape[1]), 1)
    for r in range(requests):
        mine = slice(wide_rows * r, wide_rows * (r + 1))
        dots = lax.dot_general(dec_q[mine, :].astype(bf16), cache_in[r], contract_last, preferred_element_type=f32)
        live = (place < 2 * cache_len[r]) & (lax.bitwise_and(place, 1) == 0)
        dots = jnp.where(live, dots * scale, masked_score)
        top = jnp.max(dots, axis=1, keepdims=True)
        powers = jnp.exp(dots - top)
        top_sum[0, mine, :] = jnp.broadcast_to(top, (wide_rows, HD))
        top_sum[1, mine, :] = jnp.broadcast_to(jnp.sum(powers, axis=1, keepdims=True), (wide_rows, HD))
        cached[r] = pltpu.roll(powers, 1, 1)

    for q in range(CUTS):
        crossed(zl, 0, q)
    project(zl, everything)
    take(1)
    take(2)
    sums = stat[3]
    means = sums[:, :64] / GROUP
    spreads = sums[:, 64:] / GROUP - means * means
    denoms = jnp.sqrt(jnp.maximum(spreads, variance_floor))
    in_group = lax.broadcasted_iota(jnp.int32, (16, 64), 1) == group_col
    mean_col = jnp.sum(jnp.where(in_group, means, 0.0), axis=1, keepdims=True)
    denom_col = jnp.sum(jnp.where(in_group, denoms, 0.0), axis=1, keepdims=True)
    advantage = (reward_col - mean_col) / denom_col
    block = q_in.shape[0]
    seg_row = segment[...]
    of_seq = lax.broadcasted_iota(jnp.int32, (16, block), 0) == seg_row
    coef_row = jnp.sum(jnp.where(of_seq, advantage, 0.0), axis=0, keepdims=True) * clip[...].astype(f32)
    coef_col = jnp.transpose(jnp.broadcast_to(coef_row, (HD, block)))
    seg_float = seg_row.astype(f32)
    seg_col = jnp.transpose(jnp.broadcast_to(seg_float, (HD, block)))

    q_copy.wait()
    cot_copy.wait()
    gacc[...] = jnp.zeros_like(gacc)

    def attend(i):
        here = slice(HD * i, HD * (i + 1))
        upto = HD * (i + 1)
        keys, values = acc[:upto, :HD].astype(bf16), acc[:upto, HD:].astype(bf16)
        heads = [slice(HD * h, HD * (h + 1)) for h in range(RATIO)]
        q_rows = jnp.concatenate([q_in[here, h] for h in heads], axis=0)
        coef_here = coef_col[here]
        up_rows = jnp.concatenate(
            [(coef_here * cot_in[here, h].astype(f32)).astype(bf16) for h in heads], axis=0
        )
        u_place = lax.broadcasted_iota(jnp.int32, (upto, HD), 0)
        t_place = lax.broadcasted_iota(jnp.int32, (upto, HD), 1) + HD * i
        allowed = (seg_col[:upto] == seg_float[:, here]) & (u_place <= t_place)
        bias = jnp.where(allowed, 0.0, masked_score)
        scores = lax.dot_general(keys, q_rows, contract_last, preferred_element_type=f32)
        scores = scores * scale + jnp.concatenate([bias] * RATIO, axis=1)
        top = jnp.max(scores, axis=0, keepdims=True)
        weights = jnp.exp(scores - top)
        attention = weights * (1.0 / jnp.sum(weights, axis=0, keepdims=True))
        grad_prob = lax.dot_general(values, up_rows, contract_last, preferred_element_type=f32)
        inner = jnp.sum(attention * grad_prob, axis=0, keepdims=True)
        grad_score = (attention * (grad_prob - inner) * scale).astype(bf16)
        gacc[:upto, :HD] += jnp.dot(grad_score, q_rows, preferred_element_type=f32)
        gacc[:upto, HD:] += jnp.dot(attention.astype(bf16), up_rows, preferred_element_type=f32)

    for q in range(CUTS):
        here = pl.ds(span * q, span)
        pass_on(3, q)
        hand_over(3, q)

        @pl.when(zl == 3)
        def _():
            crossed(0, 3, q)
            project(0, here)

        @pl.when(zl == 0)
        def _():
            crossed(3, 6, q)
            project(3, here)

        attend(q)

    grad_kv = gacc[...].astype(bf16)

    def outer(half):
        def step(j, carry):
            product = lax.dot_general(
                tokens[j, half], grad_kv, (((0,), (0,)), ((), ())), preferred_element_type=f32
            ).astype(bf16)
            for h in range(2):
                part[h, j, pl.ds(2 * half, 2)] = product[:, HD * h : HD * (h + 1)].reshape(2, 4, 80, HD)
            return carry

        lax.fori_loop(0, 4, step, 0)

    far = rot(zh, 2)
    near = lambda p: p + 1 - 2 * lax.rem(p, 2)
    order_of = (far, near(far), near(zh), zh)
    ring = lambda axis, half, land: Reduce(axis, half, land, sends, recvs, spot)
    direct = lambda axis, block, land: DirectReduce(axis, block, land, sends, recvs, spot)
    one, two, one_to, two_to = [], [], [], []
    for n, p in enumerate(order_of):
        one.append(
            Both(
                ring("y", lambda i, h, p=p: part.at[0, pair(h), p, i], lambda k, h, n=n: land_k.at[n, k]),
                ring("x", lambda i, h, p=p: part.at[1, i, p, pair(h)], lambda k, h, n=n: land_v.at[n, k]),
            )
        )
        one_to.append((lambda h, p=p: sum_k.at[pair(h), p], lambda h, p=p: sum_v.at[p, pair(h)]))
        two.append(
            Both(
                direct("x", lambda i, p=p: sum_k.at[i, p], lambda k, n=n: land_k_two.at[n, k]),
                direct("y", lambda i, p=p: sum_v.at[p, i], lambda k, n=n: land_v_two.at[n, k]),
            )
        )
        two_to.append((sum_two.at[0, p], sum_two.at[1, p]))
    first_z = spot.take(3)
    to_zh = [
        remote(sum_two.at[:, p], land_z.at[n], sends, recvs, first_z + n, "zh", p) for n, p in enumerate(order_of[:3])
    ]

    outer(lax.div(far, 2))
    one[0].start()
    outer(lax.div(zh, 2))
    one[1].start()
    one[0].forward()
    one[2].start()
    one[0].finish(one_to[0])
    two[0].start()
    one[1].forward()
    one[3].start()
    one[1].finish(one_to[1])
    two[1].start()
    two[0].finish(two_to[0])
    to_zh[0].start()
    one[2].forward()
    one[2].finish(one_to[2])
    two[2].start()
    one[3].forward()
    two[1].finish(two_to[1])
    to_zh[1].start()
    two[2].finish(two_to[2])
    to_zh[2].start()
    one[3].finish(one_to[3])
    two[3].start()
    two[3].finish(two_to[3])
    for copy in to_zh:
        copy.wait_recv()
    for h in range(2):
        total = sum_two[h, zh].astype(f32)
        for n in range(3):
            total = total + land_z[n, h].astype(f32)
        grads[y, h] = total

    def update(start, h, grad):
        rows_here = pl.ds(start + h, 80, stride=2)
        first = beta_one * m_one[rows_here, :] + (1.0 - beta_one) * grad
        second = beta_two * m_two[rows_here, :] + (1.0 - beta_two) * grad * grad
        old = weight[rows_here, :]
        first_hat = first / (1.0 - beta_one**adam_step)
        second_hat = second / (1.0 - beta_two**adam_step)
        new = old - learn_rate * (first_hat / (jnp.sqrt(second_hat) + adam_epsilon) + weight_decay * old)
        return rows_here, new, first, second

    for h in range(2):
        w_new[h, x, zh, y] = update(y * 160, h, grads[y, h])[1].astype(bf16)
    pieces = (zh, rot(zh, -1), rot(zh, 1), far)
    new_rows = GatherRows(w_new, pieces, sends, recvs, spot)
    small, large = new_rows.small, new_rows.large
    all_grads = Gather("y", lambda j: grads.at[j], lambda j, h: grads.at[j, h], sends, recvs, spot)
    fresh_total = jnp.zeros((dec_wide.shape[0], 2 * HD), f32)

    def fresh_of(p):
        added = jnp.zeros((dec_wide.shape[0], 2 * HD), f32)
        for i in range(4):
            columns = jnp.concatenate([w_new[h, i, p].reshape(320, HD) for h in range(2)], axis=1)
            added += jnp.dot(dec_cut[4 * i + p], columns, preferred_element_type=f32)
        return added

    new_rows.deep.start()
    small[0].start()
    all_grads.start()
    small[0].finish()
    large[0].start()
    all_grads.forward()
    new_rows.deep.forward()
    new_rows.deep.near()
    small[1].start()
    small[2].start()
    large[0].forward()
    small[1].finish()
    large[1].start()
    small[2].finish()
    large[2].start()
    all_grads.finish()
    for quarter in range(4):
        for h in range(2):
            rows_here, new, first, second = update(160 * quarter, h, grads[quarter, h])
            results[0, rows_here, :] = new
            results[1, rows_here, :] = first
            results[2, rows_here, :] = second
    outs = [
        pltpu.make_async_copy(results.at[k], ref, local.at[7 + k])
        for k, ref in enumerate((weight_out, one_out, two_out))
    ]
    for copy in outs:
        copy.start()
    new_rows.deep.last()
    small[3].start()
    large[0].finish()
    large[1].forward()
    small[3].finish()
    large[3].start()
    large[2].forward()
    fresh_total += fresh_of(pieces[0])
    large[1].finish()
    fresh_total += fresh_of(pieces[1])
    large[3].forward()
    large[2].finish()
    fresh_total += fresh_of(pieces[2])
    large[3].finish()
    fresh_total += fresh_of(pieces[3])

    fresh = fresh_total.astype(bf16)
    recent = lax.dot_general(dec_q[...].astype(bf16), fresh[:, :HD], contract_last, preferred_element_type=f32)
    row = lax.broadcasted_iota(jnp.int32, recent.shape, 0)
    column = lax.broadcasted_iota(jnp.int32, recent.shape, 1)
    first_row = lax.div(column, steps) * wide_rows
    seen = (row >= first_row) & (row < first_row + wide_rows)
    seen = seen & (lax.rem(column, steps) <= lax.bitwise_and(row, 7))
    recent = jnp.where(seen, recent * scale, masked_score)
    old_top = top_sum[0, :, :1]
    top = jnp.maximum(old_top, jnp.max(recent, axis=1, keepdims=True))
    shrink = jnp.exp(old_top - top)
    powers = jnp.exp(recent - top)
    total = top_sum[1, :, :1] * shrink + jnp.sum(powers, axis=1, keepdims=True)
    by_fresh = jnp.dot((powers / total).astype(bf16), fresh[:, HD:], preferred_element_type=f32)
    factor = shrink / total
    for r in range(requests):
        mine = slice(wide_rows * r, wide_rows * (r + 1))
        dec_weights = (cached[r] * factor[mine]).astype(bf16)
        result = by_fresh[mine] + jnp.dot(dec_weights, cache_in[r], preferred_element_type=f32)
        for h in range(RATIO):
            dec_out[r, :, HD * h : HD * (h + 1)] = result[8 * h : 8 * h + steps].astype(bf16)

    for copy in outs:
        copy.wait()
    for group in stat_copies:
        for copy in group:
            copy.wait_send()
    for q in range(CUTS):
        shard_across(zl, 0, q).wait_send()
        for d in range(3):

            @pl.when((zl >= d) & (zl < 3))
            def _():
                shard_right(d, q).wait_send()

            @pl.when((zl + d <= 3) & (zl > 0))
            def _():
                shard_left(d, q).wait_send()

        for d in (1, 2, 3):

            @pl.when(zl >= d)
            def _():
                shard_across(zl - d, d, q).wait_send()

            @pl.when(zl + d <= 3)
            def _():
                shard_across(zl + d, 3 + d, q).wait_send()

    for copy in to_zh:
        copy.wait_send()
    for group in [rows, new_rows, all_grads] + one + two:
        group.drain()


def learner(*operands):
    hidden, dec, dec_queries, kv_cache = operands[0], operands[10], operands[11], operands[12]
    anywhere = pl.BlockSpec(memory_space=pl.ANY)
    vmem = pl.BlockSpec(memory_space=pltpu.VMEM)
    block, features = hidden.shape
    requests = dec.shape[0]
    full = (2, 4, 4, 4, 80, HD)
    low = lambda *shape: pltpu.VMEM(shape, bf16)
    wide = lambda *shape: pltpu.VMEM(shape, f32)
    return pl.pallas_call(
        learner_kernel,
        out_shape=(
            jax.ShapeDtypeStruct((640, HD), f32),
            jax.ShapeDtypeStruct((640, HD), f32),
            jax.ShapeDtypeStruct((640, HD), f32),
            jax.ShapeDtypeStruct(dec_queries.shape, bf16),
        ),
        in_specs=[anywhere] * 3 + [vmem] * 5 + [anywhere] * 3 + [vmem, anywhere, pl.BlockSpec(memory_space=pltpu.SMEM)],
        out_specs=(anywhere,) * 3 + (vmem,),
        scratch_shapes=[
            low(4, 2, block, features),
            low(*full),
            low(*full),
            low(*full),
            wide(block, 2 * HD),
            wide(block, 2 * HD),
            low(block, features),
            low(block, features),
            wide(640, HD),
            wide(640, HD),
            low(*dec.shape),
            wide(requests * dec.shape[1], dec.shape[2]),
            low(16, requests * dec.shape[1], 320),
            low(*kv_cache.shape),
            wide(requests * 8 * RATIO, HD),
            wide(requests, 8 * RATIO, kv_cache.shape[1]),
            wide(2, requests * 8 * RATIO, HD),
            wide(4, 1, HD),
            wide(3, 3, 1, HD),
            low(4, 6, 2, 80, HD),
            low(4, 6, 2, 80, HD),
            low(4, 4, 80, HD),
            low(4, 4, 80, HD),
            low(4, 3, 80, HD),
            low(4, 3, 80, HD),
            low(2, 4, 80, HD),
            low(3, 2, 80, HD),
            wide(4, 2, 80, HD),
            wide(3, 640, HD),
            pltpu.SemaphoreType.DMA((10,)),
            pltpu.SemaphoreType.DMA((SEMS,)),
            pltpu.SemaphoreType.DMA((SEMS,)),
        ],
        compiler_params=pltpu.CompilerParams(collective_id=0, has_side_effects=True),
        name="learner",
    )(*operands)


def put_kernel(*refs):
    count = (len(refs) - 1) // 2
    copies = [pltpu.make_async_copy(refs[k], refs[count + k], refs[-1].at[k]) for k in range(count)]
    for copy in copies:
        copy.start()
    for copy in copies:
        copy.wait()


def put(*arrays):
    return pl.pallas_call(
        put_kernel,
        out_shape=[jax.ShapeDtypeStruct(array.shape, array.dtype) for array in arrays],
        in_specs=[pl.BlockSpec(memory_space=pltpu.VMEM)] * len(arrays),
        out_specs=[pl.BlockSpec(memory_space=pltpu.HBM)] * len(arrays),
        scratch_shapes=[pltpu.SemaphoreType.DMA((len(arrays),))],
        name="put",
    )(*arrays)


def body(
    hidden,
    queries,
    cotangent,
    segment,
    clip_mask,
    rewards,
    seq_order,
    kv_weight,
    moment_one,
    moment_two,
    dec_hidden,
    dec_queries,
    kv_cache,
    cache_len,
):
    block_rows = hidden.shape[0]
    fold = lambda value: value.reshape(-1, HD)
    requests, capacity = kv_cache.shape[:2]
    results = learner(
        hidden,
        queries,
        cotangent,
        segment,
        clip_mask.reshape(1, block_rows),
        rewards.reshape(1, -1),
        seq_order.reshape(1, -1),
        fold(kv_weight),
        fold(moment_one),
        fold(moment_two),
        dec_hidden,
        dec_queries,
        kv_cache.reshape(requests, 2 * capacity, HD),
        cache_len,
    )
    *updated, dec_out = put(*results)
    return (*(value.reshape(kv_weight.shape) for value in updated), dec_out)


def solution(mesh):
    finer = Mesh(mesh.devices.reshape(4, 4, 4, 2, 4), AXES)
    in_specs = (
        P(FSDP_POOL, TENSOR),
        P(FSDP_POOL, TENSOR),
        P(FSDP_POOL, TENSOR),
        P(FSDP_POOL, None),
        P(FSDP_POOL),
        P(FSDP_POOL),
        P(FSDP_POOL),
        P(FSDP, None, TENSOR),
        P(FSDP, None, TENSOR),
        P(FSDP, None, TENSOR),
        P(FSDP_POOL, None, None),
        P(FSDP_POOL, None, TENSOR),
        P(FSDP_POOL, None, None, TENSOR),
        P(FSDP_POOL),
    )
    out_specs = (
        P(FSDP, None, TENSOR),
        P(FSDP, None, TENSOR),
        P(FSDP, None, TENSOR),
        P(FSDP_POOL, None, TENSOR),
    )
    return jax.shard_map(body, mesh=finer, in_specs=in_specs, out_specs=out_specs, check_vma=False)
```
